32 devices in a mesh: blk: 8 (over z, x), lat: 4 (over y, core).
Axes of the slice: x: 2, y: 2, z: 4, core: 2. Of those that a mesh axis runs over, the one named last changes fastest.
Arguments:
- displacement: float32 [3, 5, 5, 5, 8, 8, 128], P(None, None, None, None, 'blk', 'lat'), may hold values from -6 to 6
- velocity: float32 [3, 5, 5, 5, 8, 8, 128], P(None, None, None, None, 'blk', 'lat'), may hold values from -6 to 6
- rigidity: float32 [5, 5, 5, 8, 8, 128], P(None, None, None, 'blk', 'lat'), may hold values from 0.5 to 2
- density: float32 [5, 5, 5, 8, 8, 128], P(None, None, None, 'blk', 'lat'), may hold values from 0.5 to 2
- history: float32 [256, 63, 3, 128], P(('blk', 'lat')), may hold values from -0.12 to 0.12
- kernel: float32 [64, 3, 3, 128], replicated, may hold values from -0.4375 to 0.4375
- owner_order: int32 [256], replicated, may hold values from 0 to 255, each once
- rigid_offset: float32 [3], replicated, may hold values from -1.8 to 1.8
- rigid_velocity: float32 [3], replicated, may hold values from -6 to 6
Outputs:
- new_displacement: float32 [3, 5, 5, 5, 8, 8, 128], P(None, None, None, None, 'blk', 'lat')
- new_velocity: float32 [3, 5, 5, 5, 8, 8, 128], P(None, None, None, None, 'blk', 'lat')
- new_history: float32 [256, 63, 3, 128], P(('blk', 'lat'))
- new_offset: float32 [3], replicated
- new_rigid_velocity: float32 [3], replicated
The draws below stay inside these ranges and needn't reach their ends.
Inputs may be any that keep to these rules, and one draw needn't show every extreme that they name: owner_order names every column 0 to 255 once; row j of history belongs to column owner_order[j].
All inputs are finite; a program needn't handle non-finite values.
Results may differ from the reference program's by a relative error of at most 0.0003.
Values sent between devices are 32-bit elements; how exact they have to be, the bound alone decides.
No kernel may reach another device: no remote copies, remote signals or barrier semaphores. Data moves between devices by JAX's collectives and lax.ppermute only.
A program may use at most 64 MiB of HBM per device.

```python
import math
import jax
import jax.numpy as jnp
import numpy as np
from jax import lax

L = 128
LAGS = 64
STEPS = 3
EZ = 128
NXE = 8
NYE = 8
COLS = 256


def level_of(key, dims, cuts, smallest, high):
    level, own = 1.0, jax.random.fold_in(key, 6)
    for dim, blocks in cuts:
        draws = jnp.exp(jax.random.uniform(jax.random.fold_in(own, dim), (blocks,), jnp.float32, smallest / len(cuts), high / len(cuts)))
        level = level * jnp.repeat(draws, dims[dim] // blocks).reshape([-1 if axis == dim else 1 for axis in range(len(dims))])
    return level


def normal_values(key, dims, width, most, cuts=(), kind=jnp.bfloat16):
    entries = jax.random.normal(key, dims, jnp.float32) * width
    if len(cuts) > 0:
        entries = level_of(key, dims, cuts, -0.22, 0.18) * entries
    return jnp.clip(entries, min=-most, max=most).astype(kind)


def setup_inputs(seed: int = 0) -> dict:
    key_of = jax.random.split(jax.random.key(seed), 10)
    displacement = normal_values(key_of[0], (3, 5, 5, 5, NXE, NYE, EZ), 1.0, 6.0, ((4, 8), (5, 4)), jnp.float32)
    velocity = normal_values(key_of[1], (3, 5, 5, 5, NXE, NYE, EZ), 1.0, 6.0, ((4, 8), (5, 4)), jnp.float32)
    rigidity = jnp.clip(jnp.exp(math.log(2.0) - 1.3862944 * jax.random.uniform(key_of[2], (5, 5, 5, NXE, NYE, EZ), jnp.float32) ** level_of(key_of[2], (5, 5, 5, NXE, NYE, EZ), ((3, 8), (4, 4)), -0.2, 0.2)), 0.5, 2.0)
    density = jnp.clip(jnp.exp(math.log(2.0) - 1.3862944 * jax.random.uniform(key_of[3], (5, 5, 5, NXE, NYE, EZ), jnp.float32) ** level_of(key_of[3], (5, 5, 5, NXE, NYE, EZ), ((3, 8), (4, 4)), -0.2, 0.2)), 0.5, 2.0)
    history = normal_values(key_of[4], (COLS, LAGS - 1, 3, L), 0.02, 0.12, ((0, 32),), jnp.float32)
    kernel = normal_values(key_of[5], (LAGS, 3, 3, L), (3 * LAGS) ** -0.5, 0.4375, (), jnp.float32)
    owner_order = jax.random.permutation(key_of[6], COLS).astype(jnp.int32)
    rigid_offset = normal_values(key_of[7], (3,), 0.3, 1.8, (), jnp.float32)
    rigid_velocity = normal_values(key_of[8], (3,), 1.0, 6.0, (), jnp.float32)
    return {"displacement": displacement, "velocity": velocity, "rigidity": rigidity, "density": density, "history": history, "kernel": kernel, "owner_order": owner_order, "rigid_offset": rigid_offset, "rigid_velocity": rigid_velocity}


pole_gap = 0.1
time_step = 0.03
rigid_gain = 20.0
coupling = 1.0
highest = lax.Precision.HIGHEST

def node_tables():
    points = np.array([-1.0, -math.sqrt(3.0 / 7.0), 0.0, math.sqrt(3.0 / 7.0), 1.0])
    weights = np.array([0.1, 49.0 / 90.0, 32.0 / 45.0, 49.0 / 90.0, 0.1])
    products = np.array([np.prod([points[row_at] - points[others] for others in range(5) if others != row_at]) for row_at in range(5)])
    slopes = np.zeros((5, 5))
    for row_at in range(5):
        for col_at in range(5):
            if row_at == col_at:
                slopes[row_at, col_at] = sum((1.0 / (points[row_at] - points[others]) for others in range(5) if others != row_at))
            else:
                slopes[row_at, col_at] = products[row_at] / products[col_at] / (points[row_at] - points[col_at])
    return (points, weights, slopes)

def node_volume():
    points, weights, slopes = node_tables()
    node_weight = jnp.asarray(weights, dtype=jnp.float32)
    volume = node_weight[:, None, None] * node_weight[None, :, None] * node_weight[None, None, :]
    return volume[:, :, :, None, None, None]

def stiffness(values, rigidity):
    points, weights, slopes = node_tables()
    deriv = jnp.asarray(slopes, dtype=jnp.float32)
    scaled = (node_volume() * rigidity)[None]
    first_dir = jnp.einsum('ia,kabcxyz->kibcxyz', deriv, values, precision=highest) * scaled
    second_dir = jnp.einsum('jb,kabcxyz->kajcxyz', deriv, values, precision=highest) * scaled
    third_dir = jnp.einsum('lc,kabcxyz->kablxyz', deriv, values, precision=highest) * scaled
    result = jnp.einsum('ia,kibcxyz->kabcxyz', deriv, first_dir, precision=highest)
    result = result + jnp.einsum('jb,kajcxyz->kabcxyz', deriv, second_dir, precision=highest)
    return result + jnp.einsum('lc,kablxyz->kabcxyz', deriv, third_dir, precision=highest)

def join_faces(lower, upper, before_first, after_last, axis):
    count = lower.shape[axis]
    earlier = jnp.concatenate((before_first, lax.slice_in_dim(upper, 0, count - 1, axis=axis)), axis=axis)
    later = jnp.concatenate((lax.slice_in_dim(lower, 1, count, axis=axis), after_last), axis=axis)
    return (lower + earlier, upper + later)

def assemble_whole(forces):
    lower, upper = (forces[:, 0], forces[:, 4])
    count = lower.shape[3]
    lower, upper = join_faces(lower, upper, lax.slice_in_dim(upper, count - 1, count, axis=3), lax.slice_in_dim(lower, 0, 1, axis=3), 3)
    forces = forces.at[:, 0].set(lower).at[:, 4].set(upper)
    lower, upper = (forces[:, :, 0], forces[:, :, 4])
    empty = jnp.zeros_like(lax.slice_in_dim(lower, 0, 1, axis=4))
    lower, upper = join_faces(lower, upper, empty, empty, 4)
    forces = forces.at[:, :, 0].set(lower).at[:, :, 4].set(upper)
    lower, upper = (forces[:, :, :, 0], forces[:, :, :, 4])
    empty = jnp.zeros_like(lax.slice_in_dim(lower, 0, 1, axis=5))
    lower, upper = join_faces(lower, upper, empty, empty, 5)
    return forces.at[:, :, :, 0].set(lower).at[:, :, :, 4].set(upper)

def interface_grid(row_first, row_count, col_first, col_count, lat_elems, lon_elems):
    points, weights, slopes = node_tables()
    nodes = jnp.asarray(points, dtype=jnp.float32)
    node_weight = jnp.asarray(weights, dtype=jnp.float32)
    theta_step = (math.pi - 2.0 * pole_gap) / lat_elems
    phi_step = 2.0 * math.pi / lon_elems
    row_elem = (row_first + jnp.arange(5 * row_count, dtype=jnp.int32) // 5).astype(jnp.float32)
    col_elem = (col_first + jnp.arange(5 * col_count, dtype=jnp.int32) // 5).astype(jnp.float32)
    colatitude = pole_gap + (row_elem + 0.5 * (1.0 + jnp.tile(nodes, row_count))) * theta_step
    longitude = (col_elem + 0.5 * (1.0 + jnp.tile(nodes, col_count))) * phi_step
    row_weight = jnp.tile(node_weight, row_count)
    col_weight = jnp.tile(node_weight, col_count)
    area_weight = 0.25 * theta_step * phi_step * (row_weight * jnp.sin(colatitude))[:, None] * col_weight[None, :]
    face_weight = row_weight[:, None] * col_weight[None, :]
    return (colatitude, longitude, area_weight, face_weight)

def rotation(colatitude, longitude):
    sin_theta = jnp.sin(colatitude)[:, None]
    cos_theta = jnp.cos(colatitude)[:, None]
    sin_phi = jnp.sin(longitude)[None, :]
    cos_phi = jnp.cos(longitude)[None, :]
    filled = jnp.ones((colatitude.shape[0], longitude.shape[0]), jnp.float32)
    radial = (sin_theta * cos_phi, sin_theta * sin_phi, cos_theta * filled)
    polar_dir = (cos_theta * cos_phi, cos_theta * sin_phi, -sin_theta * filled)
    azimuth = (-sin_phi * filled, cos_phi * filled, 0.0 * filled)
    return jnp.stack([jnp.stack([radial[axis_at], polar_dir[axis_at], azimuth[axis_at]]) for axis_at in range(3)])

def legendre(colatitude, degrees):
    cosine = jnp.cos(colatitude)[:, None]
    sine = jnp.sin(colatitude)[:, None]
    orders = jnp.arange(degrees, dtype=jnp.float32)[None, :]
    factor = jnp.where(orders == 0, math.sqrt(0.5), -jnp.sqrt((2.0 * orders + 1.0) / jnp.maximum(2.0 * orders, 1.0)) * sine)
    diagonal = jnp.cumprod(factor, axis=1)

    def advance(state_pair, degree):
        previous, before = state_pair
        level = degree.astype(jnp.float32)
        upward = jnp.sqrt(jnp.maximum(4.0 * level * level - 1.0, 0.0) / jnp.maximum(level * level - orders * orders, 1.0))
        lowered = (level - 1.0) * (level - 1.0)
        downward = jnp.sqrt(jnp.maximum(lowered - orders * orders, 0.0) / jnp.maximum(4.0 * lowered - 1.0, 1.0))
        recurred = upward * (cosine * previous - downward * before)
        values = jnp.where(orders == level, diagonal, jnp.where(orders + 1.0 == level, jnp.sqrt(2.0 * orders + 3.0) * cosine * diagonal, jnp.where(orders + 1.0 < level, recurred, 0.0)))
        return ((values, previous), values)
    zeroed = jnp.zeros((colatitude.shape[0], degrees), jnp.float32)
    finals, levels = lax.scan(advance, (zeroed, zeroed), jnp.arange(degrees, dtype=jnp.int32))
    return levels

def doubled(colatitude, degrees):
    levels = legendre(colatitude, degrees)
    return jnp.concatenate((levels, levels), axis=2)

def circle_table(longitude, degrees):
    orders = jnp.arange(degrees, dtype=jnp.float32)[None, :]
    angles = longitude[:, None] * orders
    cosines = jnp.where(orders == 0, 1.0 / math.sqrt(2.0 * math.pi), jnp.cos(angles) / math.sqrt(math.pi))
    sines = jnp.where(orders == 0, 0.0, jnp.sin(angles) / math.sqrt(math.pi))
    return jnp.concatenate((cosines, sines), axis=1)

def project(relative, area_weight, circle, levels):
    fourier = jnp.einsum('ktf,fc->ktc', relative * area_weight, circle, precision=highest)
    return jnp.einsum('ktc,ltc->ckl', fourier, levels, precision=highest)

def synthesize(coeffs, circle, levels):
    partial_value = jnp.einsum('ckl,ltc->ktc', coeffs, levels, precision=highest)
    return jnp.einsum('ktc,fc->ktf', partial_value, circle, precision=highest)

def respond(owned_rows, history, kernel):
    stacked = jnp.concatenate((owned_rows[:, None], history), axis=1)
    replies = jnp.einsum('jabl,cjbl->cal', kernel, stacked, precision=highest)
    return (replies, stacked[:, :-1])

def to_grid(values):
    bottom = values[:, :, :, 0, :, :, 0]
    lon_count, lat_count = (bottom.shape[3], bottom.shape[4])
    return bottom.transpose(0, 4, 2, 3, 1).reshape(3, 5 * lat_count, 5 * lon_count)

def from_grid(grid, lon_count, lat_count):
    return grid.reshape(3, lat_count, 5, lon_count, 5).transpose(0, 4, 2, 3, 1)

def reference(displacement, velocity, rigidity, density, history, kernel, owner_order, rigid_offset, rigid_velocity):
    lon_elems, lat_elems = (displacement.shape[4], displacement.shape[5])
    degrees = kernel.shape[3]
    colatitude, longitude, area_weight, face_weight = interface_grid(0, lat_elems, 0, lon_elems, lat_elems, lon_elems)
    rotated = rotation(colatitude, longitude)
    levels = doubled(colatitude, degrees)
    circle = circle_table(longitude, degrees)
    inverse = 1.0 / assemble_whole((density * node_volume())[None])
    for step_index in range(STEPS):
        relative = to_grid(displacement) - jnp.einsum('jktf,j->ktf', rotated, rigid_offset, precision=highest)
        partial_value = project(relative, area_weight, circle, levels)
        ordered = jnp.take(partial_value, owner_order, axis=0)
        replies, history = respond(ordered, history, kernel)
        coeffs = jnp.zeros_like(replies).at[owner_order].set(replies)
        traction = synthesize(coeffs, circle, levels)
        pull_sum = jnp.einsum('jktf,ktf->j', rotated * area_weight, traction, precision=highest)
        rigid_velocity = rigid_velocity + time_step * rigid_gain * pull_sum
        rigid_offset = rigid_offset + time_step * rigid_velocity
        forces = -stiffness(displacement, rigidity)
        forces = forces.at[:, :, :, 0, :, :, 0].add(from_grid(-coupling * face_weight * traction, lon_elems, lat_elems))
        velocity = velocity + time_step * assemble_whole(forces) * inverse
        displacement = displacement + time_step * velocity
    return (displacement, velocity, history, rigid_offset, rigid_velocity)
```

```python
import functools
import math

import jax
import jax.numpy as jnp
import numpy as np
from jax import lax
from jax.experimental import pallas as pl
from jax.experimental.pallas import tpu as pltpu
from jax.sharding import PartitionSpec as P

STEPS = 3
pole_gap = 0.1
time_step = 0.03
rigid_gain = 20.0
highest = lax.Precision.HIGHEST
f32 = jnp.float32
ROWS = 8
N3 = 125
CHUNKS = 8
HEAD = 32
PAY = HEAD + 4 * CHUNKS


def node_tables():
    points = np.array([-1.0, -math.sqrt(3.0 / 7.0), 0.0, math.sqrt(3.0 / 7.0), 1.0])
    weights = np.array([0.1, 49.0 / 90.0, 32.0 / 45.0, 49.0 / 90.0, 0.1])
    products = np.array(
        [np.prod([points[i] - points[j] for j in range(5) if j != i]) for i in range(5)]
    )
    slopes = np.zeros((5, 5))
    for i in range(5):
        for j in range(5):
            if i == j:
                slopes[i, j] = sum(1.0 / (points[i] - points[n]) for n in range(5) if n != i)
            else:
                slopes[i, j] = products[i] / products[j] / (points[i] - points[j])
    return points, weights, slopes


POINTS, WEIGHTS, SLOPES = node_tables()
VOLUME = [
    float(WEIGHTS[a] * WEIGHTS[b] * WEIGHTS[c])
    for a in range(5)
    for b in range(5)
    for c in range(5)
]


def centro_apply(matrix, x):
    s0, s1, d0, d1 = x[0] + x[4], x[1] + x[3], x[0] - x[4], x[1] - x[3]
    even, odd = [], []
    for i in range(2):
        even.append(
            (0.5 * float(matrix[i][0] + matrix[i][4])) * s0
            + (0.5 * float(matrix[i][1] + matrix[i][3])) * s1
            + float(matrix[i][2]) * x[2]
        )
    for i in range(3):
        odd.append(
            (0.5 * float(matrix[i][0] - matrix[i][4])) * d0
            + (0.5 * float(matrix[i][1] - matrix[i][3])) * d1
        )
    return [odd[0] + even[0], odd[1] + even[1], odd[2], odd[1] - even[1], odd[0] - even[0]]


def row_ids(shape):
    return lax.broadcasted_iota(jnp.int32, shape, len(shape) - 2)


def lane_ids(shape):
    return lax.broadcasted_iota(jnp.int32, shape, len(shape) - 1)


def stiffness(u, scaled, out, aux, ny):
    lanes = u.shape[-1]
    rows = row_ids((ROWS, lanes))
    for node in range(N3):
        x = u[node]
        spread = jnp.where(
            rows < ny,
            pltpu.roll(x, ny, 0),
            jnp.where(rows < 2 * ny, pltpu.roll(x, 2 * ny, 0), pltpu.roll(x, 3 * ny, 0)),
        )
        scaled[node] = spread * (-VOLUME[node])
    for direction in range(3):
        stride = (25, 5, 1)[direction]

        def line(i, carry, direction=direction, stride=stride):
            if direction == 0:
                base = i
            elif direction == 1:
                base = (i // 5) * 25 + i % 5
            else:
                base = i * 5
            slope = centro_apply(SLOPES, [u[base + j * stride] for j in range(5)])
            flux = [slope[j] * scaled[base + j * stride] for j in range(5)]
            force = centro_apply(SLOPES.T, flux)
            for j in range(5):
                at = base + j * stride
                if direction == 0:
                    out[at] = force[j]
                else:
                    out[at] = out[at] + force[j]
            return carry

        lax.fori_loop(0, 25, line, 0, unroll=5)
    if aux is not None:
        for node in range(N3):
            out[node] = jnp.where(rows < 3 * ny, out[node], aux[node] * VOLUME[node])


def join_rows(out, ny):
    lanes = out.shape[-1]
    y = row_ids((ROWS, lanes)) % ny
    for a in range(5):
        for c in range(5):
            low, high = a * 25 + c, a * 25 + 20 + c
            first, last = out[low], out[high]
            out[high] = last + jnp.where(y < ny - 1, pltpu.roll(first, ROWS - 1, 0), 0.0)
            out[low] = first + jnp.where(y > 0, pltpu.roll(last, 1, 0), 0.0)


def join_radius(out):
    lanes = out.shape[-1]
    z = lane_ids((ROWS, lanes))
    for ab in range(25):
        low, high = ab * 5, ab * 5 + 4
        first, last = out[low], out[high]
        out[high] = last + jnp.where(z < lanes - 1, pltpu.roll(first, lanes - 1, 1), 0.0)
        out[low] = first + jnp.where(z > 0, pltpu.roll(last, 1, 1), 0.0)


def spread_inverse(x, ny):
    rows = row_ids(x.shape)
    inverse = 1.0 / jnp.where(rows < 3 * ny, 1.0, x)
    return jnp.where(
        rows < ny,
        pltpu.roll(inverse, ny, 0),
        jnp.where(rows < 2 * ny, pltpu.roll(inverse, 2 * ny, 0), pltpu.roll(inverse, 3 * ny, 0)),
    )


def pack(source, aux, out, ny):
    for node in range(N3):
        for k in range(3):
            out[node, k * ny : (k + 1) * ny, :] = source[k, node]
        out[node, 3 * ny : 4 * ny, :] = aux[node]


def gather_kernel(
    dims, u, v, rig, dens, hist, kern, up, down, diag, cosrow, owner, out, pu, pv, wide
):
    ny, nlat, nown, rows_all, degrees = dims
    depth = u.shape[-1]
    out[...] = jnp.zeros(out.shape, f32)
    pack(u, rig, pu, ny)
    pack(v, dens, pv, ny)
    pick = jnp.where(
        row_ids((ROWS, depth)) == lane_ids((ROWS, depth)), 1.0, 0.0
    ) * jnp.where(row_ids((ROWS, depth)) < 2, 1.0, 0.0)
    for part, ref in enumerate((pu, pv)):
        flat = ref[...].reshape(N3 * ROWS, depth)
        picked = lax.dot_general(
            pick, flat, (((1,), (1,)), ((), ())), precision=highest, preferred_element_type=f32
        )
        for q in range(CHUNKS):
            width = min(128, N3 * ROWS - q * 128)
            at = HEAD + (part * CHUNKS + q) * 2
            out[at : at + 2, 0:width] = picked[0:2, q * 128 : q * 128 + width]
    lags = kern.shape[0]
    zero = jnp.zeros((3, degrees), f32)
    replies = []
    for first in range(0, nown, 4):
        js = list(range(first, min(nown, first + 4)))

        def lag_body(q, accs, js=js):
            ks = [[kern[q + n + 1, k] for k in range(3)] for n in range(3)]
            res = []
            for jj, j in enumerate(js):
                h = hist[j, q]
                for n in range(3):
                    for k in range(3):
                        res.append(accs[(jj * 3 + n) * 3 + k] + ks[n][k] * h)
            return tuple(res)

        accs = lax.fori_loop(0, lags - 3, lag_body, (zero,) * (9 * len(js)))
        accs = list(accs)
        for q in (lags - 3, lags - 2):
            for jj, j in enumerate(js):
                h = hist[j, q]
                for n in range(3):
                    if q + n + 1 < lags:
                        for k in range(3):
                            at = (jj * 3 + n) * 3 + k
                            accs[at] = accs[at] + kern[q + n + 1, k] * h
        for jj, j in enumerate(js):
            replies.append(
                [jnp.sum(accs[jj * 9 + i], axis=0, keepdims=True) for i in range(9)]
            )
    pad = [jnp.zeros((1, degrees), f32)] * (ROWS - nown)
    held = [jnp.concatenate([replies[j][i] for j in range(nown)] + pad, axis=0) for i in range(9)]
    device = lax.axis_index("blk") * nlat + lax.axis_index("lat")
    width = rows_all
    across = max(degrees, width)
    rows = row_ids((ROWS, across))
    order = jnp.zeros((ROWS, across), jnp.int32)
    for j in range(nown):
        order = jnp.where(rows == j, lax.rem(owner[device * nown + j], degrees), order)
    hot = jnp.where(order[:, 0:degrees] == lane_ids((ROWS, degrees)), 1.0, 0.0)
    contract = (((1,), (1,)), ((), ()))
    up_own = lax.dot_general(hot, up[...], contract, precision=highest, preferred_element_type=f32)
    down_own = lax.dot_general(
        hot, down[...], contract, precision=highest, preferred_element_type=f32
    )
    start = lax.dot_general(hot, diag[...], contract, precision=highest, preferred_element_type=f32)
    cosine = jnp.broadcast_to(cosrow[0:1, :], (ROWS, width))
    comp = (lane_ids((ROWS, width)) % ROWS) // ny
    which = order[:, 0:width]
    prev = jnp.zeros((ROWS, width), f32)
    before = jnp.zeros((ROWS, width), f32)
    sums = [jnp.zeros((ROWS, width), f32) for _ in range(3)]
    for level in range(degrees):
        value = up_own[:, level : level + 1] * (
            cosine * prev - down_own[:, level : level + 1] * before
        )
        value = jnp.where(which == level, start, value)
        for n in range(3):
            h = jnp.where(
                comp == 0,
                held[n * 3][:, level : level + 1],
                jnp.where(
                    comp == 1,
                    held[n * 3 + 1][:, level : level + 1],
                    held[n * 3 + 2][:, level : level + 1],
                ),
            )
            sums[n] = sums[n] + h * value
        before, prev = prev, value
    wide[...] = jnp.zeros(wide.shape, f32)
    for n in range(3):
        wide[:, n * width : (n + 1) * width] = sums[n]
    for q in range(HEAD // ROWS):
        out[q * ROWS : (q + 1) * ROWS, :] = wide[:, q * 128 : (q + 1) * 128]


def write_faces(force, left, right, low, high):
    for b in range(5):
        for c in range(5):
            left[b * 5 + c] = force[b * 5 + c]
            right[b * 5 + c] = force[100 + b * 5 + c]
    for a in range(5):
        for c in range(5):
            low[a * 5 + c] = force[a * 25 + c]
            high[a * 5 + c] = force[a * 25 + 20 + c]


def start_kernel(ny, u, v, rig, dens, pu, pv, force, left, right, low, high, scaled):
    pack(u, rig, pu, ny)
    pack(v, dens, pv, ny)
    stiffness(pu, scaled, force, pv, ny)
    join_rows(force, ny)
    join_radius(force)
    write_faces(force, left, right, low, high)


def advance_kernel(dims, first, last, *refs):
    ny, nlat, lanes = dims
    refs = list(refs)
    force, from_left, from_right, from_low, from_high, traction, pu, pv = refs[:8]
    refs = refs[8:]
    if not first:
        inverse = refs.pop(0)
    if last:
        out_u, out_v, total = refs
    else:
        new_u, new_v, new_force, left, right, low, high = refs[:7]
        refs = refs[7:]
        if first:
            inverse = refs.pop(0)
        total, scaled = refs
    lat = lax.axis_index("lat")
    rows = row_ids((ROWS, lanes))
    y = rows % ny
    z = lane_ids((ROWS, lanes))
    for node in range(N3):
        total[node] = force[node]
    for bc in range(25):
        total[bc] = total[bc] + from_left[bc]
        total[100 + bc] = total[100 + bc] + from_right[bc]
    has_low = jnp.where(lat > 0, 1, 0)
    has_high = jnp.where(lat < nlat - 1, 1, 0)
    take_low = jnp.logical_and(y == 0, jnp.full(y.shape, has_low, jnp.int32) > 0)
    take_high = jnp.logical_and(y == ny - 1, jnp.full(y.shape, has_high, jnp.int32) > 0)
    for a in range(5):
        for c in range(5):
            at = a * 25 + c
            total[at] = total[at] + jnp.where(
                take_low, pltpu.roll(from_low[a * 5 + c], ROWS - (ny - 1), 0), 0.0
            )
            total[at + 20] = total[at + 20] + jnp.where(
                take_high, pltpu.roll(from_high[a * 5 + c], ny - 1, 0), 0.0
            )
    if first:
        for node in range(N3):
            inverse[node] = spread_inverse(total[node], ny)
    for a in range(5):
        wa = float(WEIGHTS[a] * (2.0 if a in (0, 4) else 1.0))
        for b in range(5):
            tr = traction[b * ROWS : (b + 1) * ROWS, :]
            if tr.shape[1] != lanes:
                tr = tr[:, 0:lanes]
            moved = pltpu.roll(tr, lanes - a, 1) if a else tr
            at = a * 25 + b * 5
            total[at] = total[at] - (wa * pick_face(b, rows, ny, has_low, has_high)) * jnp.where(
                z == 0, moved, 0.0
            )
    for node in range(N3):
        speed = pv[node] + time_step * total[node] * inverse[node]
        place = pu[node] + time_step * speed
        if last:
            for k in range(3):
                out_v[k, node] = speed[k * ny : (k + 1) * ny, :]
                out_u[k, node] = place[k * ny : (k + 1) * ny, :]
        else:
            new_v[node] = speed
            new_u[node] = jnp.where(rows < 3 * ny, place, pu[node])
    if not last:
        stiffness(new_u, scaled, new_force, None, ny)
        join_rows(new_force, ny)
        join_radius(new_force)
        write_faces(new_force, left, right, low, high)


def pick_face(b, rows, ny, has_low, has_high):
    weight = float(WEIGHTS[b])
    y = rows % ny
    if b == 0:
        shared = jnp.logical_or(y > 0, jnp.full(y.shape, has_low, jnp.int32) > 0)
    elif b == 4:
        shared = jnp.logical_or(y < ny - 1, jnp.full(y.shape, has_high, jnp.int32) > 0)
    else:
        return weight
    return jnp.where(shared, 2.0 * weight, weight)


def unpack(pieces, part, rows_ref, out, dims):
    ny, nlat, nblk, lanes = dims
    count = nblk * nlat
    rows_ref[...] = jnp.zeros(rows_ref.shape, f32)
    for q in range(CHUNKS):
        for ez in range(2):
            at = ez * count
            for ref in pieces:
                n = ref.shape[0] // PAY
                rows_ref[q, at : at + n, :] = ref[
                    pl.ds(HEAD + (part * CHUNKS + q) * 2 + ez, n, stride=PAY), :
                ]
                at += n
    for q in range(CHUNKS):
        nodes = min(16, N3 - q * 16)
        for strip in range(lanes // 128):
            block = rows_ref[q, strip * 128 : (strip + 1) * 128, :].T
            out[q * 16 : q * 16 + nodes, :, strip * 128 : (strip + 1) * 128] = block[
                : nodes * ROWS
            ].reshape(nodes, ROWS, 128)


def split3(x):
    hi = x.astype(jnp.bfloat16)
    rest = x - hi.astype(f32)
    mid = rest.astype(jnp.bfloat16)
    low = (rest - mid.astype(f32)).astype(jnp.bfloat16)
    return hi, mid, low


def place_matrix(a, dims, fs):
    ny, nlat, nblk, lanes = dims
    shape = (lanes, nlat * fs)
    lam = row_ids(shape)
    col = lane_ids(shape)
    target = lax.rem(lam, nlat) * fs + lax.div(lam, nlat) * 5 + a
    hit = jnp.logical_and(col == target, lam < nlat * nblk)
    return jnp.where(hit, 1.0, 0.0).astype(jnp.bfloat16)


def lat_of(i, nlat):
    return lax.rem(lax.axis_index("lat") + i, nlat)


def to_traction(dims, n, u, tables, state, xv, hist, coef_refs, coef_out, hat, shat, xv_out, out):
    ny, nlat, nblk, lanes = dims
    legendre, circle, rowc, lanec, kern = tables
    degrees = legendre.shape[-1]
    fs = circle.shape[0]
    grid = jnp.zeros((5 * ROWS, nlat * fs), f32)
    for a in range(5):
        rows = jnp.concatenate([u[a * 25 + b * 5] for b in range(5)], axis=0)
        place = place_matrix(a, dims, fs)
        for piece in split3(rows):
            grid = grid + jnp.dot(piece, place, preferred_element_type=f32)
    cosphi, sinphi, wphi = lanec[0:1, :], lanec[1:2, :], lanec[2:3, :]
    x0, x1, x2 = xv[0:1, 0:1], xv[1:2, 0:1], xv[2:3, 0:1]
    along = x0 * cosphi + x1 * sinphi
    across = x1 * cosphi - x0 * sinphi
    for i in range(nlat):
        sl = slice(i * 5 * ROWS, (i + 1) * 5 * ROWS)
        ca, cc, cz, at = (rowc[sl, j : j + 1] for j in range(4))
        rigid = ca * along + cc * across + cz * x2
        weighted = (grid[:, i * fs : (i + 1) * fs] - rigid) * at * wphi
        hat[sl, :] = jnp.dot(
            weighted, circle[...], precision=highest, preferred_element_type=f32
        )
    blocks = degrees // ROWS
    spots = [(i, b, y) for i in range(nlat) for b in range(5) for y in range(ny)]
    zero = jnp.zeros((ROWS, degrees), f32)

    def rows_of(ref, i, b, y, k, part):
        r = (i * 5 + b) * ROWS + k * ny + y
        return ref[r : r + 1, part * degrees : (part + 1) * degrees]

    base = [lat_of(i, nlat) * (5 * ny) for i in range(nlat)]

    def analyse(blk, carry):
        l0 = pl.multiple_of(blk * (2 * ROWS), 2 * ROWS)
        accs = [[zero] * 6 for _ in range(2)]
        for i, b, y in spots:
            t = base[i] + y * 5 + b
            p = [legendre[t, pl.ds(l0 + h * ROWS, ROWS), :] for h in range(2)]
            for k in range(3):
                for part in range(2):
                    value = rows_of(hat, i, b, y, k, part)
                    for h in range(2):
                        accs[h][k * 2 + part] = accs[h][k * 2 + part] + p[h] * value
        for h in range(2):
            sl = pl.ds(l0 + h * ROWS, ROWS)
            for kp in range(6):
                coef_out[kp, sl, :] = accs[h][kp]
            for k in range(3):
                for part in range(2):
                    total = zero
                    for s, ref in enumerate([None] + coef_refs):
                        for m in range(3):
                            value = accs[h][m * 2 + part] if s == 0 else ref[m * 2 + part, sl, :]
                            col = (s * 3 + k) * 3 + m
                            total = total + kern[sl, col : col + 1] * value
                    state[k * 2 + part, sl, :] = total
        return carry

    lax.fori_loop(0, blocks // 2, analyse, 0)
    ids = row_ids((ROWS, degrees))
    for i in range(nlat):

        def synth(b, carry, i=i):
            accs = [[zero] * 6 for _ in range(ny)]
            for blk in range(blocks):
                sl = slice(blk * ROWS, (blk + 1) * ROWS)
                held = [state[kp, sl, :] for kp in range(6)]
                for y in range(ny):
                    p = legendre[base[i] + y * 5 + b, sl, :]
                    for kp in range(6):
                        accs[y][kp] = accs[y][kp] + p * held[kp]
            for part in range(2):
                block = zero
                for k in range(3):
                    for y in range(ny):
                        row = jnp.sum(accs[y][k * 2 + part], axis=0, keepdims=True)
                        block = jnp.where(ids == k * ny + y, row, block)
                shat[
                    pl.ds(pl.multiple_of((i * 5 + b) * ROWS, ROWS), ROWS),
                    part * degrees : (part + 1) * degrees,
                ] = block
            return carry

        lax.fori_loop(0, 5, synth, 0)
    traction = lax.dot_general(
        shat[...],
        circle[...],
        (((1,), (1,)), ((), ())),
        precision=highest,
        preferred_element_type=f32,
    )
    count = nlat * 5 * ROWS
    earlier = [
        hist[pl.ds(pl.multiple_of(n * count + lat_of(i, nlat) * (5 * ROWS), ROWS), 5 * ROWS), :]
        for i in range(nlat)
    ]
    traction = traction + jnp.concatenate(earlier, axis=0)
    out[...] = traction
    ca, cc, cz, at = (rowc[:, j : j + 1] for j in range(4))
    weighted = traction * at * wphi
    radial = jnp.sum(weighted * ca, axis=0, keepdims=True)
    turning = jnp.sum(weighted * cc, axis=0, keepdims=True)
    polar = jnp.sum(weighted * cz, axis=0, keepdims=True)
    pulls = [
        jnp.sum(radial * cosphi - turning * sinphi, axis=1, keepdims=True),
        jnp.sum(radial * sinphi + turning * cosphi, axis=1, keepdims=True),
        jnp.sum(polar, axis=1, keepdims=True),
    ]
    for j in range(3):
        speed = xv[3 + j : 4 + j, :] + time_step * rigid_gain * pulls[j]
        xv_out[3 + j : 4 + j, :] = speed
        xv_out[j : j + 1, :] = xv[j : j + 1, :] + time_step * speed
    xv_out[6:8, :] = jnp.zeros((2, xv_out.shape[1]), f32)


def first_interface(dims, npieces, *refs):
    ny, nlat, nblk, lanes = dims
    pieces = refs[:npieces]
    tables, order_circle, xv = refs[npieces : npieces + 5], refs[npieces + 5], refs[npieces + 6]
    u, hist, coef, xv_out, out = refs[npieces + 7 : npieces + 12]
    rows_ref, held, state, hat, shat = refs[npieces + 12 :]
    unpack(pieces, 0, rows_ref, u, dims)
    at = 0
    for ref in pieces:
        for d in range(ref.shape[0] // PAY):
            for q in range(HEAD // ROWS):
                held[at : at + ROWS, q * 128 : (q + 1) * 128] = ref[
                    d * PAY + q * ROWS : d * PAY + (q + 1) * ROWS, :
                ]
            at += ROWS
    hist[...] = lax.dot_general(
        held[:, 0 : hist.shape[0]],
        order_circle[...],
        (((0,), (0,)), ((), ())),
        precision=highest,
        preferred_element_type=f32,
    )
    to_traction(dims, 0, u, tables, state, xv, hist, [], coef, hat, shat, xv_out, out)


def interface_force(dims, u, aux, scaled, force):
    ny, nlat, nblk, lanes = dims
    count = nlat * nblk
    stiffness(u, scaled, force, aux, ny)
    join_rows(force, ny)
    shape = (ROWS, lanes)
    lam = lane_ids(shape)
    rows = row_ids(shape)
    y = rows % ny
    lat_at = lax.rem(lam, nlat)
    blk_at = lax.rem(lax.div(lam, nlat), nblk)
    for ab in range(25):
        high = ab * 5 + 4
        force[high] = force[high] + jnp.where(
            lam < count, pltpu.roll(force[ab * 5], lanes - count, 1), 0.0
        )
    wrap = count - nlat
    for bc in range(25):
        first, last = force[bc], force[100 + bc]
        lower = jnp.where(
            blk_at == 0, pltpu.roll(last, lanes - wrap, 1), pltpu.roll(last, nlat, 1)
        )
        upper = jnp.where(
            blk_at == nblk - 1, pltpu.roll(first, wrap, 1), pltpu.roll(first, lanes - nlat, 1)
        )
        force[bc] = first + lower
        force[100 + bc] = last + upper
    absolute = lax.rem(lat_at + lax.axis_index("lat"), nlat)
    take_low = jnp.logical_and(y == 0, absolute > 0)
    take_high = jnp.logical_and(y == ny - 1, absolute < nlat - 1)
    for a in range(5):
        for c in range(5):
            low, high = a * 25 + c, a * 25 + 20 + c
            first, last = force[low], force[high]
            lower = jnp.where(
                lat_at == 0, pltpu.roll(last, lanes - (nlat - 1), 1), pltpu.roll(last, 1, 1)
            )
            upper = jnp.where(
                lat_at == nlat - 1, pltpu.roll(first, nlat - 1, 1), pltpu.roll(first, lanes - 1, 1)
            )
            force[low] = first + jnp.where(
                take_low, pltpu.roll(lower, ROWS - (ny - 1), 0), 0.0
            )
            force[high] = last + jnp.where(take_high, pltpu.roll(upper, ny - 1, 0), 0.0)


def add_traction(dims, traction, force, fs):
    ny, nlat, nblk, lanes = dims
    shape = (ROWS, lanes)
    lam = lane_ids(shape)
    rows = row_ids(shape)
    absolute = lax.rem(lax.rem(lam, nlat) + lax.axis_index("lat"), nlat)
    y = rows % ny
    grid = jnp.concatenate(
        [traction[i * 5 * ROWS : (i + 1) * 5 * ROWS, :] for i in range(nlat)], axis=1
    )
    parts = split3(grid)
    for a in range(5):
        place = place_matrix(a, dims, fs)
        moved = jnp.zeros((5 * ROWS, lanes), f32)
        for piece in parts:
            moved = moved + lax.dot_general(
                piece, place, (((1,), (1,)), ((), ())), preferred_element_type=f32
            )
        wa = float(WEIGHTS[a] * (2.0 if a in (0, 4) else 1.0))
        for b in range(5):
            weight = float(WEIGHTS[b]) * wa
            if b == 0:
                shared = jnp.logical_or(y > 0, absolute > 0)
            elif b == 4:
                shared = jnp.logical_or(y < ny - 1, absolute < nlat - 1)
            else:
                shared = None
            face = weight if shared is None else jnp.where(shared, 2.0 * weight, weight)
            at = a * 25 + b * 5
            force[at] = force[at] - face * moved[b * ROWS : (b + 1) * ROWS]


def second_interface(dims, npieces, *refs):
    ny, nlat, nblk, lanes = dims
    pieces = refs[:npieces]
    tables = refs[npieces : npieces + 5]
    xv, hist, u, coef0, traction = refs[npieces + 5 : npieces + 10]
    new_u, new_v, inverse, coef, xv_out, out = refs[npieces + 10 : npieces + 16]
    rows_ref, state, hat, shat, force, scaled, v = refs[npieces + 16 :]
    unpack(pieces, 1, rows_ref, v, dims)
    interface_force(dims, u, v, scaled, force)
    rows = row_ids((ROWS, lanes))
    lam = lane_ids((ROWS, lanes))
    for node in range(N3):
        mass = force[node]
        inverse[node] = spread_inverse(jnp.where(lam < nlat * nblk, mass, 1.0), ny)
    add_traction(dims, traction, force, tables[1].shape[0])
    for node in range(N3):
        speed = v[node] + time_step * force[node] * inverse[node]
        new_v[node] = speed
        new_u[node] = jnp.where(rows < 3 * ny, u[node] + time_step * speed, u[node])
    to_traction(dims, 1, new_u, tables, state, xv, hist, [coef0], coef, hat, shat, xv_out, out)


def third_interface(dims, *refs):
    ny, nlat, nblk, lanes = dims
    tables = refs[:5]
    xv, hist, u, v, inverse, coef1, coef0, traction, owner = refs[5:14]
    xv_out, out, kept = refs[14:17]
    state, hat, shat, force, scaled, coef = refs[17:]
    interface_force(dims, u, None, scaled, force)
    add_traction(dims, traction, force, tables[1].shape[0])
    rows = row_ids((ROWS, lanes))
    for ab in range(25):
        node = ab * 5
        speed = v[node] + time_step * force[node] * inverse[node]
        scaled[node] = u[node] + time_step * speed
    to_traction(
        dims, 2, scaled, tables, state, xv, hist, [coef1, coef0], coef, hat, shat, xv_out, out
    )
    nown = kept.shape[0]
    degrees = tables[0].shape[-1]
    device = lax.axis_index("blk") * nlat + lax.axis_index("lat")
    ids = row_ids((ROWS, 2 * degrees))
    column = jnp.full((ROWS, 2 * degrees), -1, jnp.int32)
    for j in range(nown):
        column = jnp.where(ids == j, owner[device * nown + j], column)
    hot = jnp.where(column == lane_ids((ROWS, 2 * degrees)), 1.0, 0.0)
    for n, ref in enumerate((coef, coef1, coef0)):
        for k in range(3):
            both = jnp.concatenate([ref[2 * k], ref[2 * k + 1]], axis=1)
            mine = lax.dot_general(
                hot, both, (((1,), (1,)), ((), ())), precision=highest, preferred_element_type=f32
            )
            for j in range(nown):
                kept[j, n, k : k + 1, :] = mine[j : j + 1]


def legendre_tables(colatitude, degrees):
    cosine = np.cos(colatitude)[:, None]
    sine = np.sin(colatitude)[:, None]
    orders = np.arange(degrees, dtype=np.float64)[None, :]
    factor = np.where(
        orders == 0,
        math.sqrt(0.5),
        -np.sqrt((2.0 * orders + 1.0) / np.maximum(2.0 * orders, 1.0)) * sine,
    )
    diagonal = np.cumprod(factor, axis=1)
    levels = np.zeros((len(colatitude), degrees, degrees))
    ups = np.zeros((degrees, degrees))
    downs = np.zeros((degrees, degrees))
    previous = before = np.zeros((len(colatitude), degrees))
    for level in range(degrees):
        above = orders < level
        up = np.where(
            above,
            np.sqrt(
                max(4.0 * level * level - 1.0, 0.0) / np.maximum(level * level - orders**2, 1.0)
            ),
            0.0,
        )
        lowered = (level - 1.0) ** 2
        down = np.where(
            above,
            np.sqrt(np.maximum(lowered - orders**2, 0.0) / max(4.0 * lowered - 1.0, 1.0)),
            0.0,
        )
        values = up * (cosine * previous - down * before)
        values = np.where(orders == level, diagonal, values)
        levels[:, level, :] = values
        ups[level], downs[level] = up[0], down[0]
        before, previous = previous, values
    return (
        levels.astype(np.float32),
        ups.astype(np.float32),
        downs.astype(np.float32),
        diagonal.astype(np.float32),
    )


def on_device(
    mesh_sizes,
    displacement,
    velocity,
    rigidity,
    density,
    history,
    kernel,
    owner_order,
    rigid_offset,
    rigid_velocity,
):
    nblk, nlat = mesh_sizes
    nx, ny, depth = displacement.shape[4:]
    assert nx == 1 and 4 * ny == ROWS
    degrees = kernel.shape[3]
    lags = kernel.shape[0]
    nown = history.shape[0]
    lat_elems, lon_elems = ny * nlat, nblk
    nt, nf = 5 * lat_elems, 5 * lon_elems
    count = nblk * nlat
    lanes = -(-2 * count // 128) * 128
    fs = -(-nf // 128) * 128
    rows_all = nlat * 5 * ROWS
    dims = (ny, nlat, nblk, lanes)
    blk, lat = lax.axis_index("blk"), lax.axis_index("lat")

    theta_step = (math.pi - 2.0 * pole_gap) / lat_elems
    phi_step = 2.0 * math.pi / lon_elems
    theta = pole_gap + (np.arange(nt) // 5 + 0.5 * (1.0 + np.tile(POINTS, lat_elems))) * theta_step
    phi = (np.arange(nf) // 5 + 0.5 * (1.0 + np.tile(POINTS, lon_elems))) * phi_step
    table, ups, downs, diagonal = legendre_tables(theta, degrees)
    orders = np.arange(degrees)[None, :]
    angles = phi[:, None] * orders
    cosines = np.where(orders == 0, 1.0 / math.sqrt(2.0 * math.pi), np.cos(angles) / math.sqrt(math.pi))
    sines = np.where(orders == 0, 0.0, np.sin(angles) / math.sqrt(math.pi))
    circle_all = np.concatenate([cosines, sines], axis=1).astype(np.float32)
    r = np.arange(rows_all)
    r_lat, r_b, r_s = r // (5 * ROWS), (r // ROWS) % 5, r % ROWS
    r_k, r_y = r_s // ny, r_s % ny
    r_t = (r_lat * ny + r_y) * 5 + r_b
    real = r_k < 3
    th = theta[r_t]
    rowc_all = np.zeros((rows_all, 8))
    rowc_all[:, 0] = np.where(r_k == 0, np.sin(th), np.where(r_k == 1, np.cos(th), 0.0))
    rowc_all[:, 1] = np.where(r_k == 2, 1.0, 0.0)
    rowc_all[:, 2] = np.where(r_k == 0, np.cos(th), np.where(r_k == 1, -np.sin(th), 0.0))
    rowc_all[:, 3] = np.where(
        real, 0.25 * theta_step * phi_step * WEIGHTS[r_b] * np.sin(th), 0.0
    )
    lanec_all = np.zeros((8, nf))
    lanec_all[0], lanec_all[1] = np.cos(phi), np.sin(phi)
    lanec_all[2] = np.tile(WEIGHTS, lon_elems)
    diag_rows = np.where(real[:, None], diagonal[r_t], 0.0).astype(np.float32)
    cos_rows = np.where(real, np.cos(th), 0.0).astype(np.float32)

    def rolled(values, start, axis):
        both = jnp.asarray(np.concatenate([values, values], axis=axis).astype(np.float32))
        return lax.dynamic_slice_in_dim(both, start, values.shape[axis], axis)

    vmem = pl.BlockSpec(memory_space=pltpu.VMEM)
    smem = pl.BlockSpec(memory_space=pltpu.SMEM)
    def shaped(*dims_):
        return jax.ShapeDtypeStruct(dims_, f32)

    def cost(micros):
        return pl.CostEstimate(
            flops=int(micros * 5e6), transcendentals=0, bytes_accessed=int(micros * 1e6)
        )

    u4 = displacement.reshape(3, N3, ny, depth)
    v4 = velocity.reshape(3, N3, ny, depth)
    rig = rigidity.reshape(N3, ny, depth)
    dens = density.reshape(N3, ny, depth)

    payload = pl.pallas_call(
        functools.partial(gather_kernel, (ny, nlat, nown, rows_all, degrees)),
        out_shape=shaped(PAY, 128),
        in_specs=[vmem] * 10 + [smem],
        out_specs=vmem,
        scratch_shapes=[pltpu.VMEM((N3, ROWS, depth), f32)] * 2
        + [pltpu.VMEM((ROWS, 16 * HEAD), f32)],
        name="gather",
        cost_estimate=cost(6),
    )(
        u4,
        v4,
        rig,
        dens,
        history,
        kernel,
        jnp.asarray(ups),
        jnp.asarray(downs),
        jnp.asarray(diag_rows),
        jnp.asarray(np.tile(cos_rows[None], (8, 1))),
        owner_order,
    )

    def shifted(x, axis, size, by):
        return lax.ppermute(x, axis, [(s, (s - by) % size) for s in range(size)])

    column = jnp.concatenate(
        [payload] + [shifted(payload, "lat", nlat, i) for i in range(1, nlat)], axis=0
    )
    if nblk <= 8:
        pieces = [column] + [shifted(column, "blk", nblk, i) for i in range(1, nblk)]
        base_blk = blk
    else:
        pieces = [lax.all_gather(column, "blk", axis=0, tiled=True)]
        base_blk = blk * 0

    packed = shaped(N3, ROWS, depth)
    face = shaped(25, ROWS, depth)
    buffer = pltpu.VMEM((N3, ROWS, depth), f32)
    pu, pv, force, *faces = pl.pallas_call(
        functools.partial(start_kernel, ny),
        out_shape=(packed,) * 3 + (face,) * 4,
        in_specs=[vmem] * 4,
        out_specs=(vmem,) * 7,
        scratch_shapes=[buffer],
        name="forces",
        cost_estimate=cost(4),
    )(u4, v4, rig, dens)

    def exchange(left, right, low, high):
        from_left = shifted(right, "blk", nblk, -1)
        from_right = shifted(left, "blk", nblk, 1)
        low = jnp.concatenate([low[:5] + from_left[:5], low[5:20], low[20:] + from_right[:5]])
        high = jnp.concatenate([high[:5] + from_left[20:], high[5:20], high[20:] + from_right[20:]])
        return from_left, from_right, shifted(high, "lat", nlat, -1), shifted(low, "lat", nlat, 1)

    circle = rolled(circle_all, base_blk * 5, 0)
    circle = jnp.pad(circle, ((0, fs - nf), (0, 0)))
    lanec = jnp.pad(rolled(lanec_all, base_blk * 5, 1), ((0, 0), (0, fs - nf)))
    rowc = rolled(rowc_all, lat * (5 * ROWS), 0)
    owners = owner_order.reshape(nblk, nlat, nown)
    owners = lax.dynamic_slice_in_dim(jnp.concatenate([owners, owners], 0), base_blk, nblk, 0)
    owners = lax.dynamic_slice_in_dim(jnp.concatenate([owners, owners], 1), lat, nlat, 1)
    owners = jnp.pad(owners.reshape(count, nown), ((0, 0), (0, ROWS - nown)), constant_values=-1)
    owners = owners.reshape(count * ROWS)
    hot = (owners[:, None] == jnp.arange(2 * degrees, dtype=jnp.int32)[None, :]).astype(f32)
    order_circle = jnp.einsum("pc,fc->pf", hot, circle, precision=highest)
    kern = kernel[:3].reshape(27, degrees).T
    tables = (jnp.asarray(table), circle, rowc, lanec, kern)
    xv = jnp.concatenate([rigid_offset, rigid_velocity, jnp.zeros((2,), f32)])
    xv = jnp.broadcast_to(xv[:, None], (8, 128))

    wide = shaped(N3, ROWS, lanes)
    held = pltpu.VMEM((N3, ROWS, lanes), f32)
    coefs = shaped(6, degrees, degrees)
    grid_rows = shaped(rows_all, fs)
    hats = [
        pltpu.VMEM((6, degrees, degrees), f32),
        pltpu.VMEM((rows_all, 2 * degrees), f32),
        pltpu.VMEM((rows_all, 2 * degrees), f32),
    ]
    npieces = len(pieces)
    xvs = shaped(8, 128)
    gu, hist, coef0, xv1, traction0 = pl.pallas_call(
        functools.partial(first_interface, dims, npieces),
        out_shape=(wide, shaped(3 * rows_all, fs), coefs, xvs, grid_rows),
        in_specs=[vmem] * (npieces + 7),
        out_specs=(vmem,) * 5,
        scratch_shapes=[pltpu.VMEM((CHUNKS, lanes, 128), f32), pltpu.VMEM((count * ROWS, 16 * HEAD), f32)]
        + hats,
        name="interface0",
        cost_estimate=cost(8),
    )(*pieces, *tables, order_circle, xv)

    def own(traction):
        mine = traction[: 5 * ROWS]
        if nblk > 8:
            mine = lax.dynamic_slice_in_dim(mine, blk * 5, 5, 1)
            mine = jnp.pad(mine, ((0, 0), (0, depth - 5)))
        return mine

    def advance(first, last, force, moved, traction, pu, pv, inverse):
        three = shaped(3, N3, ny, depth)
        outs = (three,) * 2 if last else (packed,) * 3 + (face,) * 4 + (packed,) * first
        return pl.pallas_call(
            functools.partial(advance_kernel, (ny, nlat, depth), first, last),
            out_shape=outs,
            in_specs=[vmem] * (8 + (not first)),
            out_specs=(vmem,) * len(outs),
            scratch_shapes=[buffer] * (1 if last and not first else 2),
            name="advance",
            cost_estimate=cost(4),
        )(force, *moved, own(traction), pu, pv, *(() if first else (inverse,)))

    moved = exchange(*faces)
    pu, pv, force, *rest = advance(True, False, force, moved, traction0, pu, pv, None)
    faces, inverse = rest[:4], rest[4]
    moved = exchange(*faces)
    gu1, gv1, ginv, coef1, xv2, traction1 = pl.pallas_call(
        functools.partial(second_interface, dims, npieces),
        out_shape=(wide, wide, wide, coefs, xvs, grid_rows),
        in_specs=[vmem] * (npieces + 10),
        out_specs=(vmem,) * 6,
        scratch_shapes=[pltpu.VMEM((CHUNKS, lanes, 128), f32)] + hats + [held] * 3,
        name="interface1",
        cost_estimate=cost(8),
    )(*pieces, *tables, xv1, hist, gu, coef0, traction0)
    pu, pv, force, *faces = advance(False, False, force, moved, traction1, pu, pv, inverse)
    moved = exchange(*faces)
    xv3, traction2, kept = pl.pallas_call(
        functools.partial(third_interface, dims),
        out_shape=(xvs, grid_rows, shaped(nown, 3, 3, degrees)),
        in_specs=[vmem] * 13 + [smem],
        out_specs=(vmem,) * 3,
        scratch_shapes=hats + [held] * 2 + [pltpu.VMEM((6, degrees, degrees), f32)],
        name="interface2",
        cost_estimate=cost(8),
    )(*tables, xv2, hist, gu1, gv1, ginv, coef1, coef0, traction1, owner_order)
    new_u, new_v = advance(False, True, force, moved, traction2, pu, pv, inverse)
    new_history = jnp.concatenate([kept, history[:, : lags - 1 - STEPS]], axis=1)
    return (
        new_u.reshape(displacement.shape),
        new_v.reshape(velocity.shape),
        new_history,
        xv3[0:3, 0],
        xv3[3:6, 0],
    )


def solution(mesh):
    field = P(None, None, None, None, "blk", "lat", None)
    nodal = P(None, None, None, "blk", "lat", None)
    columns = P(("blk", "lat"), None, None, None)
    in_specs = (field, field, nodal, nodal, columns, P(), P(), P(), P())
    out_specs = (field, field, columns, P(), P())
    return jax.shard_map(
        functools.partial(on_device, (mesh.shape["blk"], mesh.shape["lat"])),
        mesh=mesh,
        in_specs=in_specs,
        out_specs=out_specs,
        check_vma=False,
    )
```

```python
import functools
import math

import jax
import jax.numpy as jnp
import numpy as np
from jax import lax
from jax.experimental import pallas as pl
from jax.experimental.pallas import tpu as pltpu
from jax.sharding import PartitionSpec as P

STEPS = 3
pole_gap = 0.1
time_step = 0.03
rigid_gain = 20.0
highest = lax.Precision.HIGHEST
f32 = jnp.float32
ROWS = 8
N3 = 125
HALF = 13
CHUNKS = 8
HEAD = 24
PAY = HEAD + 3 * CHUNKS


def node_tables():
    points = np.array([-1.0, -math.sqrt(3.0 / 7.0), 0.0, math.sqrt(3.0 / 7.0), 1.0])
    weights = np.array([0.1, 49.0 / 90.0, 32.0 / 45.0, 49.0 / 90.0, 0.1])
    products = np.array(
        [np.prod([points[i] - points[j] for j in range(5) if j != i]) for i in range(5)]
    )
    slopes = np.zeros((5, 5))
    for i in range(5):
        for j in range(5):
            if i == j:
                slopes[i, j] = sum(1.0 / (points[i] - points[n]) for n in range(5) if n != i)
            else:
                slopes[i, j] = products[i] / products[j] / (points[i] - points[j])
    return points, weights, slopes


POINTS, WEIGHTS, SLOPES = node_tables()
VOLUME = [
    float(WEIGHTS[a] * WEIGHTS[b] * WEIGHTS[c])
    for a in range(5)
    for b in range(5)
    for c in range(5)
]


def centro_apply(matrix, x):
    s0, s1, d0, d1 = x[0] + x[4], x[1] + x[3], x[0] - x[4], x[1] - x[3]
    even, odd = [], []
    for i in range(2):
        even.append(
            (0.5 * float(matrix[i][0] + matrix[i][4])) * s0
            + (0.5 * float(matrix[i][1] + matrix[i][3])) * s1
            + float(matrix[i][2]) * x[2]
        )
    for i in range(3):
        odd.append(
            (0.5 * float(matrix[i][0] - matrix[i][4])) * d0
            + (0.5 * float(matrix[i][1] - matrix[i][3])) * d1
        )
    return [odd[0] + even[0], odd[1] + even[1], odd[2], odd[1] - even[1], odd[0] - even[0]]


def row_ids(shape):
    return lax.broadcasted_iota(jnp.int32, shape, len(shape) - 2)


def lane_ids(shape):
    return lax.broadcasted_iota(jnp.int32, shape, len(shape) - 1)


def stiffness(u, scaled, out, aux, ny):
    lanes = u.shape[-1]
    rows = row_ids((ROWS, lanes))
    for node in range(N3):
        x = u[node]
        spread = jnp.where(
            rows < ny,
            pltpu.roll(x, ny, 0),
            jnp.where(rows < 2 * ny, pltpu.roll(x, 2 * ny, 0), pltpu.roll(x, 3 * ny, 0)),
        )
        scaled[node] = spread * (-VOLUME[node])
    for direction in range(3):
        stride = (25, 5, 1)[direction]

        def line(i, carry, direction=direction, stride=stride):
            if direction == 0:
                base = i
            elif direction == 1:
                base = (i // 5) * 25 + i % 5
            else:
                base = i * 5
            slope = centro_apply(SLOPES, [u[base + j * stride] for j in range(5)])
            flux = [slope[j] * scaled[base + j * stride] for j in range(5)]
            force = centro_apply(SLOPES.T, flux)
            for j in range(5):
                at = base + j * stride
                if direction == 0:
                    out[at] = force[j]
                else:
                    out[at] = out[at] + force[j]
            return carry

        lax.fori_loop(0, 25, line, 0, unroll=5)
    if aux is not None:
        for node in range(N3):
            out[node] = jnp.where(rows < 3 * ny, out[node], aux[node] * VOLUME[node])


def join_rows(out, ny):
    lanes = out.shape[-1]
    y = row_ids((ROWS, lanes)) % ny
    for a in range(5):
        for c in range(5):
            low, high = a * 25 + c, a * 25 + 20 + c
            first, last = out[low], out[high]
            out[high] = last + jnp.where(y < ny - 1, pltpu.roll(first, ROWS - 1, 0), 0.0)
            out[low] = first + jnp.where(y > 0, pltpu.roll(last, 1, 0), 0.0)


def join_radius(out):
    lanes = out.shape[-1]
    z = lane_ids((ROWS, lanes))
    for ab in range(25):
        low, high = ab * 5, ab * 5 + 4
        first, last = out[low], out[high]
        out[high] = last + jnp.where(z < lanes - 1, pltpu.roll(first, lanes - 1, 1), 0.0)
        out[low] = first + jnp.where(z > 0, pltpu.roll(last, 1, 1), 0.0)


def spread_inverse(x, ny):
    rows = row_ids(x.shape)
    inverse = 1.0 / jnp.where(rows < 3 * ny, 1.0, x)
    return jnp.where(
        rows < ny,
        pltpu.roll(inverse, ny, 0),
        jnp.where(rows < 2 * ny, pltpu.roll(inverse, 2 * ny, 0), pltpu.roll(inverse, 3 * ny, 0)),
    )


def pack(source, aux, out, ny):
    for node in range(N3):
        for k in range(3):
            out[node, k * ny : (k + 1) * ny, :] = source[k, node]
        out[node, 3 * ny : 4 * ny, :] = aux[node]


def gather_kernel(
    dims, u, v, rig, dens, hist, kern, up, down, diag, cosrow, owner, out, pu, pv, wide, turned
):
    ny, nlat, nown, rows_all, degrees = dims
    depth = u.shape[-1]
    out[...] = jnp.zeros(out.shape, f32)
    pack(u, rig, pu, ny)
    pack(v, dens, pv, ny)
    for ab in range(25):
        low, high = ab * 5, ab * 5 + 4
        above = pltpu.roll(pv[low], depth - 1, 1)
        pv[high] = pv[high] + jnp.where(row_ids((ROWS, depth)) >= 3 * ny, above, 0.0)
    lane = lane_ids((ROWS, depth))
    for n in range(16):
        merged = jnp.zeros((ROWS, depth), f32)
        for q in range(CHUNKS):
            if q * 16 + n < N3:
                x = pu[q * 16 + n]
                merged = jnp.where(lane // 2 == q, pltpu.roll(x, 2 * q, 1) if q else x, merged)
                at = 2 * CHUNKS + q
                merged = jnp.where(lane == at, pltpu.roll(pv[q * 16 + n], at, 1), merged)
        turned[n * ROWS : (n + 1) * ROWS, :] = merged
    out[HEAD:PAY, :] = turned[...].T[0 : PAY - HEAD]
    lags = kern.shape[2]
    accs = [jnp.zeros((nown, degrees), f32) for _ in range(9)]
    for lag in range(1, lags):
        for k in range(3):
            for m in range(3):
                weight = kern[k, m, lag : lag + 1, :]
                for n in range(3):
                    if lag - n - 1 >= 0:
                        accs[n * 3 + k] = accs[n * 3 + k] + weight * hist[lag - n - 1, m]
    held = accs
    if nown < ROWS:
        pad = jnp.zeros((ROWS - nown, degrees), f32)
        held = [jnp.concatenate([x, pad], axis=0) for x in accs]
    device = lax.axis_index("blk") * nlat + lax.axis_index("lat")
    width = rows_all
    across = max(degrees, width)
    rows = row_ids((ROWS, across))
    order = jnp.zeros((ROWS, across), jnp.int32)
    for j in range(nown):
        order = jnp.where(rows == j, lax.rem(owner[device * nown + j], degrees), order)
    hot = jnp.where(order[:, 0:degrees] == lane_ids((ROWS, degrees)), 1.0, 0.0)
    contract = (((1,), (1,)), ((), ()))
    up_own = lax.dot_general(hot, up[...], contract, precision=highest, preferred_element_type=f32)
    down_own = lax.dot_general(
        hot, down[...], contract, precision=highest, preferred_element_type=f32
    )
    start = lax.dot_general(hot, diag[...], contract, precision=highest, preferred_element_type=f32)
    cosine = jnp.broadcast_to(cosrow[0:1, :], (ROWS, width))
    comp = (lane_ids((ROWS, width)) % (3 * ny)) // ny
    which = order[:, 0:width]
    prev = jnp.zeros((ROWS, width), f32)
    before = jnp.zeros((ROWS, width), f32)
    sums = [jnp.zeros((ROWS, width), f32) for _ in range(3)]
    for level in range(degrees):
        value = up_own[:, level : level + 1] * (
            cosine * prev - down_own[:, level : level + 1] * before
        )
        value = jnp.where(which == level, start, value)
        for n in range(3):
            h = jnp.where(
                comp == 0,
                held[n * 3][:, level : level + 1],
                jnp.where(
                    comp == 1,
                    held[n * 3 + 1][:, level : level + 1],
                    held[n * 3 + 2][:, level : level + 1],
                ),
            )
            sums[n] = sums[n] + h * value
        before, prev = prev, value
    wide[...] = jnp.zeros(wide.shape, f32)
    for n in range(3):
        wide[:, n * width : (n + 1) * width] = sums[n]
    for q in range(HEAD // ROWS):
        out[q * ROWS : (q + 1) * ROWS, :] = wide[:, q * 128 : (q + 1) * 128]


def write_faces(force, left, right, low, high):
    for b in range(5):
        for c in range(5):
            left[b * 5 + c] = force[b * 5 + c]
            right[b * 5 + c] = force[100 + b * 5 + c]
    for a in range(5):
        for c in range(5):
            low[a * 5 + c] = force[a * 25 + c]
            high[a * 5 + c] = force[a * 25 + 20 + c]


def start_kernel(ny, u, v, rig, dens, pu, pv, force, left, right, low, high, scaled):
    pack(u, rig, pu, ny)
    pack(v, dens, pv, ny)
    stiffness(pu, scaled, force, pv, ny)
    join_rows(force, ny)
    join_radius(force)
    write_faces(force, left, right, low, high)


def fold_kernel(ny, from_left, from_right, low, high, token, out_low, out_high):
    y = row_ids(low.shape[1:]) % ny

    def full(ref, n, at):
        if n < 5:
            return ref[n] + from_left[at + n]
        return ref[n] + from_right[at + n - 20] if n >= 20 else ref[n]

    for p in range(HALF):
        first, second = full(low, p, 0), full(high, p, 20)
        if p + HALF < 25:
            first = jnp.where(y == 0, first, pltpu.roll(full(low, p + HALF, 0), 1, 0))
            second = jnp.where(y > 0, second, pltpu.roll(full(high, p + HALF, 20), ROWS - 1, 0))
        out_low[p] = first
        out_high[p] = second


def advance_kernel(dims, first, last, *refs):
    ny, nlat, lanes = dims
    refs = list(refs)
    force, from_left, from_right, from_low, from_high, traction, pu, pv = refs[:8]
    refs = refs[8:]
    if not first:
        inverse = refs.pop(0)
    if last:
        out_u, out_v, total = refs
    else:
        new_u, new_v, new_force, left, right, low, high = refs[:7]
        refs = refs[7:]
        if first:
            inverse = refs.pop(0)
        total, scaled = refs
    lat = lax.axis_index("lat")
    rows = row_ids((ROWS, lanes))
    y = rows % ny
    z = lane_ids((ROWS, lanes))
    for node in range(N3):
        total[node] = force[node]
    for bc in range(25):
        total[bc] = total[bc] + from_left[bc]
        total[100 + bc] = total[100 + bc] + from_right[bc]
    has_low = jnp.where(lat > 0, 1, 0)
    has_high = jnp.where(lat < nlat - 1, 1, 0)
    take_low = jnp.logical_and(y == 0, jnp.full(y.shape, has_low, jnp.int32) > 0)
    take_high = jnp.logical_and(y == ny - 1, jnp.full(y.shape, has_high, jnp.int32) > 0)
    for a in range(5):
        for c in range(5):
            at = a * 25 + c
            n = a * 5 + c
            if n < HALF:
                lower = pltpu.roll(from_low[n], ROWS - 1, 0)
                upper = pltpu.roll(from_high[n], 1, 0)
            else:
                lower, upper = from_low[n - HALF], from_high[n - HALF]
            total[at] = total[at] + jnp.where(take_low, lower, 0.0)
            total[at + 20] = total[at + 20] + jnp.where(take_high, upper, 0.0)
    if first:
        for node in range(N3):
            inverse[node] = spread_inverse(total[node], ny)
    for a in range(5):
        wa = float(WEIGHTS[a] * (2.0 if a in (0, 4) else 1.0))
        for b in range(5):
            tr = traction[b * ROWS : (b + 1) * ROWS, :]
            if tr.shape[1] != lanes:
                tr = tr[:, 0:lanes]
            moved = pltpu.roll(tr, lanes - a, 1) if a else tr
            at = a * 25 + b * 5
            total[at] = total[at] - (wa * pick_face(b, rows, ny, has_low, has_high)) * jnp.where(
                z == 0, moved, 0.0
            )
    for node in range(N3):
        speed = pv[node] + time_step * total[node] * inverse[node]
        place = pu[node] + time_step * speed
        if last:
            for k in range(3):
                out_v[k, node] = speed[k * ny : (k + 1) * ny, :]
                out_u[k, node] = place[k * ny : (k + 1) * ny, :]
        else:
            new_v[node] = speed
            new_u[node] = jnp.where(rows < 3 * ny, place, pu[node])
    if not last:
        stiffness(new_u, scaled, new_force, None, ny)
        join_rows(new_force, ny)
        join_radius(new_force)
        write_faces(new_force, left, right, low, high)


def pick_face(b, rows, ny, has_low, has_high):
    weight = float(WEIGHTS[b])
    y = rows % ny
    if b == 0:
        shared = jnp.logical_or(y > 0, jnp.full(y.shape, has_low, jnp.int32) > 0)
    elif b == 4:
        shared = jnp.logical_or(y < ny - 1, jnp.full(y.shape, has_high, jnp.int32) > 0)
    else:
        return weight
    return jnp.where(shared, 2.0 * weight, weight)


def unpack(pieces, part, rows_ref, out, dims):
    ny, nlat, nblk, lanes = dims
    count = nblk * nlat
    rows_ref[...] = jnp.zeros(rows_ref.shape, f32)
    for q in range(CHUNKS):
        for core, ref in enumerate(pieces):
            n = ref.shape[0] // PAY
            for ez in range(2 if part == 0 else 1):
                at = HEAD + 2 * q + ez if part == 0 else HEAD + 2 * CHUNKS + q
                rows_ref[q, pl.ds(ez * count + core, n, stride=2), :] = ref[
                    pl.ds(at, n, stride=PAY), :
                ]
    for q in range(CHUNKS):
        nodes = min(16, N3 - q * 16)
        for strip in range(lanes // 128):
            block = rows_ref[q, strip * 128 : (strip + 1) * 128, :].T
            out[q * 16 : q * 16 + nodes, :, strip * 128 : (strip + 1) * 128] = block[
                : nodes * ROWS
            ].reshape(nodes, ROWS, 128)


def split3(x):
    hi = x.astype(jnp.bfloat16)
    rest = x - hi.astype(f32)
    mid = rest.astype(jnp.bfloat16)
    low = (rest - mid.astype(f32)).astype(jnp.bfloat16)
    return hi, mid, low


def place_matrices(out, dims, fs):
    ny, nlat, nblk, lanes = dims
    lam = row_ids((lanes, fs))
    offset = lane_ids((lanes, fs)) - lax.div(lam, nlat) * 5
    for i in range(nlat):
        mine = jnp.logical_and(lax.rem(lam, nlat) == i, lam < nlat * nblk)
        at = jnp.where(mine, offset, -1)
        for a in range(5):
            out[a * lanes : (a + 1) * lanes, i * fs : (i + 1) * fs] = jnp.where(
                at == a, 1.0, 0.0
            ).astype(jnp.bfloat16)


def times_onehot(x, place, transposed):
    n = x.shape[0]
    parts = jnp.concatenate(split3(x), axis=0)
    axes = (((1,), (1 if transposed else 0,)), ((), ()))
    y = lax.dot_general(parts, place[...], axes, preferred_element_type=f32)
    return y[0:n] + y[n : 2 * n] + y[2 * n : 3 * n]


def lat_of(i, nlat):
    return lax.bitwise_xor(lax.axis_index("lat"), jnp.int32(i))


def to_traction(dims, n, u, tables, scratch, xv, hist, coef_refs, coef_out, xv_out, out):
    ny, nlat, nblk, lanes = dims
    legendre, circle, rowc, lanec, weights, kernels = tables
    state, hat, shat, mix, place, kern = scratch
    kern[...] = jnp.zeros(kern.shape, f32)
    for s in range(1 + len(coef_refs)):
        for k in range(3):
            for m in range(3):
                at = (s * 3 + k) * 3 + m
                kern[at : at + 1, :] = kernels[k, m, s : s + 1, :]
    kern[...] = kern[...].T
    degrees = legendre.shape[-1]
    fs = circle.shape[0]
    grid = times_onehot(
        jnp.concatenate(
            [
                jnp.concatenate([u[a * 25 + b * 5] for b in range(5)], axis=0)
                for a in range(5)
            ],
            axis=1,
        ),
        place,
        False,
    )
    cosphi, sinphi, wphi = lanec[0:1, :], lanec[1:2, :], weights[0:1, :]
    x0, x1, x2 = xv[0:1, 0:1], xv[1:2, 0:1], xv[2:3, 0:1]
    along = x0 * cosphi + x1 * sinphi
    across = x1 * cosphi - x0 * sinphi
    fields, columns = [], []
    for i in range(nlat):
        here = rowc[pl.ds(pl.multiple_of(lat_of(i, nlat) * (5 * ROWS), ROWS), 5 * ROWS), :]
        columns.append(here)
        ca, cc, cz, at = (here[:, j : j + 1] for j in range(4))
        rigid = ca * along + cc * across + cz * x2
        fields.append((grid[:, i * fs : (i + 1) * fs] - rigid) * at * wphi)
    hat[...] = jnp.dot(
        jnp.concatenate(fields, axis=0),
        circle[...],
        precision=highest,
        preferred_element_type=f32,
    )
    blocks = degrees // ROWS
    zero = jnp.zeros((ROWS, degrees), f32)
    ids = row_ids((ROWS, degrees))
    even = (ids + lane_ids((ROWS, degrees))) % 2 == 0
    lat = lax.axis_index("lat")
    spots = nlat // 2 * 5 * ny

    def block_starts(at, b):
        north = lax.bitwise_xor(jnp.int32(at), lat)
        south = lax.bitwise_xor(jnp.int32(nlat - 1 - at), lat)
        return (
            pl.multiple_of((north * 5 + b) * ROWS, ROWS),
            pl.multiple_of((south * 5 + 4 - b) * ROWS, ROWS),
        )

    for at in range(nlat // 2):
        for b in range(5):
            north, south = block_starts(at, b)
            for part in range(2):
                sl = slice(part * degrees, (part + 1) * degrees)
                upper, lower = hat[pl.ds(north, ROWS), sl], hat[pl.ds(south, ROWS), sl]
                lower = jnp.where(
                    ids % ny == 0, pltpu.roll(lower, ROWS - 1, 0), pltpu.roll(lower, 1, 0)
                )
                both, apart = upper + lower, upper - lower
                for k in range(3):
                    for y in range(ny):
                        r = k * ny + y
                        mix[((at * 5 + b) * ny + y) * 6 + k * 2 + part] = jnp.where(
                            even, both[r : r + 1], apart[r : r + 1]
                        )
    group = 4

    def analyse(blk, carry):
        l0 = pl.multiple_of(blk * (group * ROWS), group * ROWS)
        accs = [[zero] * 6 for _ in range(group)]
        for spot in range(spots):
            values = [mix[spot * 6 + kp] for kp in range(6)]
            for h in range(group):
                p = legendre[spot, pl.ds(l0 + h * ROWS, ROWS), :]
                for kp in range(6):
                    accs[h][kp] = accs[h][kp] + p * values[kp]
        for h in range(group):
            sl = pl.ds(l0 + h * ROWS, ROWS)
            for kp in range(6):
                coef_out[kp, sl, :] = accs[h][kp]
            for k in range(3):
                totals = [zero, zero]
                for s, ref in enumerate([None] + coef_refs):
                    for m in range(3):
                        col = (s * 3 + k) * 3 + m
                        weight = jnp.broadcast_to(kern[sl, col : col + 1], (ROWS, degrees))
                        for part in range(2):
                            kp = m * 2 + part
                            value = accs[h][kp] if s == 0 else ref[kp, sl, :]
                            totals[part] = totals[part] + weight * value
                for part in range(2):
                    state[k * 2 + part, sl, :] = totals[part]
        return carry

    lax.fori_loop(0, blocks // group, analyse, 0)

    def synth(nb, carry):
        at, b = lax.div(nb, 5), lax.rem(nb, 5)
        accs = [[zero] * 6 for _ in range(ny)]
        for blk in range(blocks):
            sl = slice(blk * ROWS, (blk + 1) * ROWS)
            held = [state[kp, sl, :] for kp in range(6)]
            for y in range(ny):
                p = legendre[nb * ny + y, sl, :]
                for kp in range(6):
                    accs[y][kp] = accs[y][kp] + p * held[kp]
        north, south = block_starts(at, b)
        for part in range(2):
            upper = lower = zero
            for k in range(3):
                for y in range(ny):
                    acc = accs[y][k * 2 + part]
                    total = jnp.sum(acc, axis=0, keepdims=True)
                    signed = jnp.sum(jnp.where(even, acc, -acc), axis=0, keepdims=True)
                    upper = jnp.where(ids == k * ny + y, total, upper)
                    lower = jnp.where(ids == k * ny + ny - 1 - y, signed, lower)
            sl = slice(part * degrees, (part + 1) * degrees)
            shat[pl.ds(north, ROWS), sl] = upper
            shat[pl.ds(south, ROWS), sl] = lower
        return carry

    lax.fori_loop(0, nlat // 2 * 5, synth, 0)
    traction = lax.dot_general(
        shat[...],
        circle[...],
        (((1,), (1,)), ((), ())),
        precision=highest,
        preferred_element_type=f32,
    )
    count = nlat * 5 * ROWS
    earlier = [
        hist[pl.ds(pl.multiple_of(n * count + lat_of(i, nlat) * (5 * ROWS), ROWS), 5 * ROWS), :]
        for i in range(nlat)
    ]
    traction = traction + jnp.concatenate(earlier, axis=0)
    out[...] = traction
    here = jnp.concatenate(columns, axis=0)
    ca, cc, cz, at = (here[:, j : j + 1] for j in range(4))
    weighted = traction * at * wphi
    radial = jnp.sum(weighted * ca, axis=0, keepdims=True)
    turning = jnp.sum(weighted * cc, axis=0, keepdims=True)
    polar = jnp.sum(weighted * cz, axis=0, keepdims=True)
    pulls = [
        jnp.sum(radial * cosphi - turning * sinphi, axis=1, keepdims=True),
        jnp.sum(radial * sinphi + turning * cosphi, axis=1, keepdims=True),
        jnp.sum(polar, axis=1, keepdims=True),
    ]
    for j in range(3):
        speed = xv[3 + j : 4 + j, :] + time_step * rigid_gain * pulls[j]
        xv_out[3 + j : 4 + j, :] = speed
        xv_out[j : j + 1, :] = xv[j : j + 1, :] + time_step * speed
    xv_out[6:8, :] = jnp.zeros((2, xv_out.shape[1]), f32)


def first_interface(dims, npieces, *refs):
    ny, nlat, nblk, lanes = dims
    pieces = refs[:npieces]
    tables, order_circle, xv = refs[npieces : npieces + 6], refs[npieces + 6], refs[npieces + 7 : npieces + 9]
    u, hist, coef, xv_out, out = refs[npieces + 9 : npieces + 14]
    rows_ref, held, start, *scratch = refs[npieces + 14 :]
    for j in range(3):
        start[j : j + 1, :] = jnp.full((1, start.shape[1]), xv[0][j], f32)
        start[3 + j : 4 + j, :] = jnp.full((1, start.shape[1]), xv[1][j], f32)
    place_matrices(scratch[4], dims, tables[1].shape[0])
    unpack(pieces, 0, rows_ref, u, dims)
    for core, ref in enumerate(pieces):
        for d in range(ref.shape[0] // PAY):
            at = (2 * d + core) * ROWS
            for q in range(HEAD // ROWS):
                held[at : at + ROWS, q * 128 : (q + 1) * 128] = ref[
                    d * PAY + q * ROWS : d * PAY + (q + 1) * ROWS, :
                ]
    group = 3 * ny
    groups = hist.shape[0] // ROWS
    summed = lax.dot_general(
        held[...],
        order_circle[...],
        (((0,), (0,)), ((), ())),
        precision=highest,
        preferred_element_type=f32,
    )
    spare = jnp.zeros((ROWS - group, summed.shape[1]), f32)
    for g in range(groups):
        hist[g * ROWS : (g + 1) * ROWS, :] = jnp.concatenate(
            [summed[g * group : (g + 1) * group], spare], axis=0
        )
    to_traction(dims, 0, u, tables, scratch, start, hist, [], coef, xv_out, out)


def interface_force(dims, u, aux, scaled, force):
    ny, nlat, nblk, lanes = dims
    count = nlat * nblk
    stiffness(u, scaled, force, aux, ny)
    join_rows(force, ny)
    shape = (ROWS, lanes)
    lam = lane_ids(shape)
    rows = row_ids(shape)
    y = rows % ny
    lat_at = lax.rem(lam, nlat)
    blk_at = lax.rem(lax.div(lam, nlat), nblk)
    for ab in range(25):
        high = ab * 5 + 4
        force[high] = force[high] + jnp.where(
            lam < count, pltpu.roll(force[ab * 5], lanes - count, 1), 0.0
        )
    wrap = count - nlat
    for bc in range(25):
        first, last = force[bc], force[100 + bc]
        lower = jnp.where(
            blk_at == 0, pltpu.roll(last, lanes - wrap, 1), pltpu.roll(last, nlat, 1)
        )
        upper = jnp.where(
            blk_at == nblk - 1, pltpu.roll(first, wrap, 1), pltpu.roll(first, lanes - nlat, 1)
        )
        force[bc] = first + lower
        force[100 + bc] = last + upper
    absolute = lax.bitwise_xor(lat_at, jnp.full(shape, lax.axis_index("lat"), jnp.int32))
    take_low = jnp.logical_and(y == 0, absolute > 0)
    take_high = jnp.logical_and(y == ny - 1, absolute < nlat - 1)

    def neighbour(x, by_one):
        back, ahead = pltpu.roll(x, 1, 1), pltpu.roll(x, lanes - 1, 1)
        far = jnp.where(lat_at == 0, pltpu.roll(x, lanes - 3, 1), pltpu.roll(x, 3, 1))
        middle = jnp.logical_or(lat_at == 1, lat_at == 2)
        one = jnp.where(lat_at % 2 == 0, ahead, back)
        three = jnp.where(middle, jnp.where(lat_at == 1, ahead, back), far)
        return jnp.where(by_one, one, three)

    for a in range(5):
        for c in range(5):
            low, high = a * 25 + c, a * 25 + 20 + c
            first, last = force[low], force[high]
            lower = neighbour(last, absolute % 2 == 1)
            upper = neighbour(first, absolute % 2 == 0)
            force[low] = first + jnp.where(
                take_low, pltpu.roll(lower, ROWS - (ny - 1), 0), 0.0
            )
            force[high] = last + jnp.where(take_high, pltpu.roll(upper, ny - 1, 0), 0.0)


def add_traction(dims, traction, force, place):
    ny, nlat, nblk, lanes = dims
    shape = (ROWS, lanes)
    lam = lane_ids(shape)
    rows = row_ids(shape)
    absolute = lax.bitwise_xor(lax.rem(lam, nlat), jnp.full(shape, lax.axis_index("lat"), jnp.int32))
    y = rows % ny
    grid = jnp.concatenate(
        [traction[i * 5 * ROWS : (i + 1) * 5 * ROWS, :] for i in range(nlat)], axis=1
    )
    spread = times_onehot(grid, place, True)
    for a in range(5):
        moved = spread[:, a * lanes : (a + 1) * lanes]
        wa = float(WEIGHTS[a] * (2.0 if a in (0, 4) else 1.0))
        for b in range(5):
            weight = float(WEIGHTS[b]) * wa
            if b == 0:
                shared = jnp.logical_or(y > 0, absolute > 0)
            elif b == 4:
                shared = jnp.logical_or(y < ny - 1, absolute < nlat - 1)
            else:
                shared = None
            face = weight if shared is None else jnp.where(shared, 2.0 * weight, weight)
            at = a * 25 + b * 5
            force[at] = force[at] - face * moved[b * ROWS : (b + 1) * ROWS]


def second_interface(dims, npieces, *refs):
    ny, nlat, nblk, lanes = dims
    pieces = refs[:npieces]
    u, traction, new_u, new_v, inverse, rows_ref, force, scaled, v, place = refs[npieces:]
    place_matrices(place, dims, traction.shape[1])
    unpack(pieces, 1, rows_ref, v, dims)
    interface_force(dims, u, v, scaled, force)
    rows = row_ids((ROWS, lanes))
    lam = lane_ids((ROWS, lanes))
    for node in range(N3):
        mass = force[node]
        inverse[node] = spread_inverse(jnp.where(lam < nlat * nblk, mass, 1.0), ny)
    add_traction(dims, traction, force, place)
    for node in range(N3):
        speed = v[node] + time_step * force[node] * inverse[node]
        new_v[node] = speed
        new_u[node] = jnp.where(rows < 3 * ny, u[node] + time_step * speed, u[node])


def second_traction(dims, *refs):
    tables, (xv, hist, u, coef0) = refs[:6], refs[6:10]
    coef, xv_out, out, *scratch = refs[10:]
    place_matrices(scratch[4], dims, tables[1].shape[0])
    to_traction(dims, 1, u, tables, scratch, xv, hist, [coef0], coef, xv_out, out)


def third_interface(dims, u, v, inverse, traction, new_u, force, scaled, place):
    place_matrices(place, dims, traction.shape[1])
    interface_force(dims, u, None, scaled, force)
    add_traction(dims, traction, force, place)
    for ab in range(25):
        node = ab * 5
        speed = v[node] + time_step * force[node] * inverse[node]
        new_u[node] = u[node] + time_step * speed


def third_traction(dims, *refs):
    ny, nlat, nblk, lanes = dims
    tables, (xv, hist, u, coef1, coef0, owner) = refs[:6], refs[6:12]
    xv_out, out, kept, coef, *scratch = refs[12:]
    place_matrices(scratch[4], dims, tables[1].shape[0])
    to_traction(dims, 2, u, tables, scratch, xv, hist, [coef1, coef0], coef, xv_out, out)
    nown = kept.shape[2]
    degrees = tables[0].shape[-1]
    device = lax.axis_index("blk") * nlat + lax.axis_index("lat")
    ids = row_ids((ROWS, 2 * degrees))
    column = jnp.full((ROWS, 2 * degrees), -1, jnp.int32)
    for j in range(nown):
        column = jnp.where(ids == j, owner[device * nown + j], column)
    hot = jnp.where(column == lane_ids((ROWS, 2 * degrees)), 1.0, 0.0)
    for n, ref in enumerate((coef, coef1, coef0)):
        for k in range(3):
            both = jnp.concatenate([ref[2 * k], ref[2 * k + 1]], axis=1)
            mine = lax.dot_general(
                hot, both, (((1,), (1,)), ((), ())), precision=highest, preferred_element_type=f32
            )
            kept[n, k] = mine[0:nown]


def legendre_tables(colatitude, degrees):
    cosine = np.cos(colatitude)[:, None]
    sine = np.sin(colatitude)[:, None]
    orders = np.arange(degrees, dtype=np.float64)[None, :]
    factor = np.where(
        orders == 0,
        math.sqrt(0.5),
        -np.sqrt((2.0 * orders + 1.0) / np.maximum(2.0 * orders, 1.0)) * sine,
    )
    diagonal = np.cumprod(factor, axis=1)
    levels = np.zeros((len(colatitude), degrees, degrees))
    ups = np.zeros((degrees, degrees))
    downs = np.zeros((degrees, degrees))
    previous = before = np.zeros((len(colatitude), degrees))
    for level in range(degrees):
        above = orders < level
        up = np.where(
            above,
            np.sqrt(
                max(4.0 * level * level - 1.0, 0.0) / np.maximum(level * level - orders**2, 1.0)
            ),
            0.0,
        )
        lowered = (level - 1.0) ** 2
        down = np.where(
            above,
            np.sqrt(np.maximum(lowered - orders**2, 0.0) / max(4.0 * lowered - 1.0, 1.0)),
            0.0,
        )
        values = up * (cosine * previous - down * before)
        values = np.where(orders == level, diagonal, values)
        levels[:, level, :] = values
        ups[level], downs[level] = up[0], down[0]
        before, previous = previous, values
    return (
        levels.astype(np.float32),
        ups.astype(np.float32),
        downs.astype(np.float32),
        diagonal.astype(np.float32),
    )


def on_device(
    mesh_sizes,
    displacement,
    velocity,
    rigidity,
    density,
    history,
    kernel,
    owner_order,
    rigid_offset,
    rigid_velocity,
):
    nblk, nlat = mesh_sizes
    nx, ny, depth = displacement.shape[4:]
    degrees = kernel.shape[3]
    lags = kernel.shape[0]
    nown = history.shape[0]
    lat_elems, lon_elems = ny * nlat, nblk
    nt, nf = 5 * lat_elems, 5 * lon_elems
    count = nblk * nlat
    lanes = -(-2 * count // 128) * 128
    fs = -(-nf // 128) * 128
    rows_all = nlat * 5 * ROWS
    hist_rows = nlat * 5 * 3 * ny
    assert nx == 1 and 4 * ny == ROWS and nlat == 4 and 3 * hist_rows <= 16 * HEAD
    dims = (ny, nlat, nblk, lanes)
    blk, lat = lax.axis_index("blk"), lax.axis_index("lat")

    theta_step = (math.pi - 2.0 * pole_gap) / lat_elems
    phi_step = 2.0 * math.pi / lon_elems
    theta = pole_gap + (np.arange(nt) // 5 + 0.5 * (1.0 + np.tile(POINTS, lat_elems))) * theta_step
    phi = (np.arange(nf) // 5 + 0.5 * (1.0 + np.tile(POINTS, lon_elems))) * phi_step
    table, ups, downs, diagonal = legendre_tables(theta, degrees)
    orders = np.arange(degrees)[None, :]
    angles = phi[:, None] * orders
    cosines = np.where(orders == 0, 1.0 / math.sqrt(2.0 * math.pi), np.cos(angles) / math.sqrt(math.pi))
    sines = np.where(orders == 0, 0.0, np.sin(angles) / math.sqrt(math.pi))
    circle_all = np.concatenate([cosines, sines], axis=1).astype(np.float32)
    r = np.arange(rows_all)
    r_lat, r_b, r_s = r // (5 * ROWS), (r // ROWS) % 5, r % ROWS
    r_k, r_y = r_s // ny, r_s % ny
    r_t = (r_lat * ny + r_y) * 5 + r_b
    real = r_k < 3
    th = theta[r_t]
    rowc_all = np.zeros((rows_all, 8))
    rowc_all[:, 0] = np.where(r_k == 0, np.sin(th), np.where(r_k == 1, np.cos(th), 0.0))
    rowc_all[:, 1] = np.where(r_k == 2, 1.0, 0.0)
    rowc_all[:, 2] = np.where(r_k == 0, np.cos(th), np.where(r_k == 1, -np.sin(th), 0.0))
    rowc_all[:, 3] = np.where(
        real, 0.25 * theta_step * phi_step * WEIGHTS[r_b] * np.sin(th), 0.0
    )
    lanec_all = np.zeros((8, nf))
    lanec_all[0], lanec_all[1] = np.cos(phi), np.sin(phi)
    lanec_all[2] = np.tile(WEIGHTS, lon_elems)
    diag_rows = diagonal[r_t[real]]
    cos_rows = np.cos(th[real]).astype(np.float32)

    spot = np.arange(nt // 2)
    spot_t = (spot // (5 * ny) * ny + spot % ny) * 5 + spot // ny % 5
    north = jnp.asarray(table[spot_t])
    vmem = pl.BlockSpec(memory_space=pltpu.VMEM)
    smem = pl.BlockSpec(memory_space=pltpu.SMEM)
    def shaped(*dims_):
        return jax.ShapeDtypeStruct(dims_, f32)

    def cost(micros):
        return pl.CostEstimate(
            flops=int(micros * 5e6), transcendentals=0, bytes_accessed=int(micros * 1e6)
        )

    u4 = displacement.reshape(3, N3, ny, depth)
    v4 = velocity.reshape(3, N3, ny, depth)
    rig = rigidity.reshape(N3, ny, depth)
    dens = density.reshape(N3, ny, depth)
    past = history.transpose(1, 2, 0, 3)

    payload = pl.pallas_call(
        functools.partial(gather_kernel, (ny, nlat, nown, hist_rows, degrees)),
        out_shape=shaped(PAY, 128),
        in_specs=[vmem] * 10 + [smem],
        out_specs=vmem,
        scratch_shapes=[pltpu.VMEM((N3, ROWS, depth), f32)] * 2
        + [pltpu.VMEM((ROWS, 16 * HEAD), f32), pltpu.VMEM((16 * ROWS, depth), f32)],
        name="gather",
        cost_estimate=cost(6),
    )(
        u4,
        v4,
        rig,
        dens,
        past,
        kernel.transpose(1, 2, 0, 3),
        jnp.asarray(ups),
        jnp.asarray(downs),
        jnp.asarray(diag_rows),
        jnp.asarray(np.tile(cos_rows[None], (8, 1))),
        owner_order,
    )

    def shifted(x, axis, size, by):
        return lax.ppermute(x, axis, [(s, (s - by) % size) for s in range(size)])

    def swapped(x, bit):
        return lax.ppermute(x, "lat", [(i, i ^ bit) for i in range(nlat)])

    column = jnp.concatenate([payload, swapped(payload, 2)], axis=0)
    if nblk <= 8:
        mine = [column] + [shifted(column, "blk", nblk, i) for i in range(1, nblk)]
        mine = jnp.concatenate(mine, axis=0)
        base_blk = blk
    else:
        mine = lax.all_gather(column, "blk", axis=0, tiled=True)
        base_blk = blk * 0
    packed = shaped(N3, ROWS, depth)
    face = shaped(25, ROWS, depth)
    buffer = pltpu.VMEM((N3, ROWS, depth), f32)
    pu, pv, force, *faces = pl.pallas_call(
        functools.partial(start_kernel, ny),
        out_shape=(packed,) * 3 + (face,) * 4,
        in_specs=[vmem] * 4,
        out_specs=(vmem,) * 7,
        scratch_shapes=[buffer],
        name="forces",
        cost_estimate=cost(4),
    )(u4, v4, rig, dens)
    *faces, column_seen = lax.optimization_barrier((*faces, column))

    def exchange_lon(left, right):
        return shifted(right, "blk", nblk, -1), shifted(left, "blk", nblk, 1)

    def exchange_lat(from_left, from_right, low, high, token):
        half = shaped(HALF, ROWS, depth)
        low, high = pl.pallas_call(
            functools.partial(fold_kernel, ny),
            out_shape=(half,) * 2,
            in_specs=[vmem] * 4 + [pl.BlockSpec(memory_space=pl.ANY)],
            out_specs=(vmem,) * 2,
            name="fold",
            cost_estimate=cost(1),
        )(from_left, from_right, low, high, token)
        received = shifted(high, "lat", nlat, -1), shifted(low, "lat", nlat, 1)
        return (from_left, from_right, *received), low


    def turned(values, axis):
        reach = np.take(values, np.arange(nf + fs) % nf, axis=axis).astype(np.float32)
        return lax.dynamic_slice_in_dim(jnp.asarray(reach), base_blk * 5, fs, axis)

    circle = turned(circle_all, 0)
    lanec = turned(lanec_all, 1)
    wphi = np.zeros((8, fs), np.float32)
    wphi[0, :nf] = np.tile(WEIGHTS, lon_elems)
    rowc = jnp.asarray(rowc_all.astype(np.float32))
    owners = owner_order.reshape(nblk, nlat, nown)
    owners = lax.dynamic_slice_in_dim(jnp.concatenate([owners, owners], 0), base_blk, nblk, 0)
    owners = jnp.take(owners, lax.bitwise_xor(lat, jnp.arange(nlat, dtype=jnp.int32)), axis=1)
    owners = jnp.pad(owners.reshape(count, nown), ((0, 0), (0, ROWS - nown)), constant_values=-1)
    owners = owners.reshape(count * ROWS)
    hot = (owners[:, None] == jnp.arange(2 * degrees, dtype=jnp.int32)[None, :]).astype(f32)
    order_circle = jnp.einsum("pc,fc->pf", hot, circle, precision=highest)
    tables = (north, circle, rowc, lanec, jnp.asarray(wphi), kernel.transpose(1, 2, 0, 3))

    wide = shaped(N3, ROWS, lanes)
    held = pltpu.VMEM((N3, ROWS, lanes), f32)
    coefs = shaped(6, degrees, degrees)
    grid_rows = shaped(rows_all, fs)
    hats = [
        pltpu.VMEM((6, degrees, degrees), f32),
        pltpu.VMEM((rows_all, 2 * degrees), f32),
        pltpu.VMEM((rows_all, 2 * degrees), f32),
        pltpu.VMEM((nlat // 2 * 5 * ny * 6, ROWS, degrees), f32),
        pltpu.VMEM((5 * lanes, nlat * fs), jnp.bfloat16),
        pltpu.VMEM((degrees, 128), f32),
    ]
    npieces = 2
    xvs = shaped(8, 128)
    *lon, mine = lax.optimization_barrier((*exchange_lon(*faces[:2]), mine))
    pieces = [mine, swapped(mine, 1)]
    moved, folded = exchange_lat(*lon, *faces[2:], column_seen)
    first_offset, folded = lax.optimization_barrier((rigid_offset, folded))
    gu, hist, coef0, xv1, traction0 = pl.pallas_call(
        functools.partial(first_interface, dims, npieces),
        out_shape=(wide, shaped(3 * rows_all, fs), coefs, xvs, grid_rows),
        in_specs=[vmem] * (npieces + 7) + [smem] * 2,
        out_specs=(vmem,) * 5,
        scratch_shapes=[pltpu.VMEM((CHUNKS, lanes, 128), f32), pltpu.VMEM((count * ROWS, 16 * HEAD), f32)]
        + [pltpu.VMEM((8, 128), f32)]
        + hats,
        name="interface0",
        cost_estimate=cost(8),
    )(*pieces, *tables, order_circle, first_offset, rigid_velocity)

    def own(traction):
        mine = traction
        if nblk > 8:
            mine = traction[: 5 * ROWS]
            mine = lax.dynamic_slice_in_dim(mine, blk * 5, 5, 1)
            mine = jnp.pad(mine, ((0, 0), (0, depth - 5)))
        return mine

    def advance(first, last, force, moved, traction, pu, pv, inverse):
        three = shaped(3, N3, ny, depth)
        outs = (three,) * 2 if last else (packed,) * 3 + (face,) * 4 + (packed,) * first
        return pl.pallas_call(
            functools.partial(advance_kernel, (ny, nlat, depth), first, last),
            out_shape=outs,
            in_specs=[vmem] * (8 + (not first)),
            out_specs=(vmem,) * len(outs),
            scratch_shapes=[buffer] * (1 if last and not first else 2),
            name="advance",
            cost_estimate=cost(4),
        )(force, *moved, own(traction), pu, pv, *(() if first else (inverse,)))

    pu, pv, force, *rest = advance(True, False, force, moved, traction0, pu, pv, None)
    faces, inverse = rest[:4], rest[4]
    gu, left_seen = lax.optimization_barrier((gu, faces[0]))
    place = pltpu.VMEM((5 * lanes, nlat * fs), jnp.bfloat16)
    gu1, gv1, ginv = pl.pallas_call(
        functools.partial(second_interface, dims, npieces),
        out_shape=(wide,) * 3,
        in_specs=[vmem] * (npieces + 2),
        out_specs=(vmem,) * 3,
        scratch_shapes=[pltpu.VMEM((CHUNKS, lanes, 128), f32)] + [held] * 3 + [place],
        name="interface1",
        cost_estimate=cost(4),
    )(*pieces, gu, traction0)
    moved, folded = exchange_lat(*exchange_lon(*faces[:2]), *faces[2:], gv1)
    xv1, folded = lax.optimization_barrier((xv1, folded))
    coef1, xv2, traction1 = pl.pallas_call(
        functools.partial(second_traction, dims),
        out_shape=(coefs, xvs, grid_rows),
        in_specs=[vmem] * 10,
        out_specs=(vmem,) * 3,
        scratch_shapes=hats,
        name="traction1",
        cost_estimate=cost(5),
    )(*tables, xv1, hist, gu1, coef0)
    pu, pv, force, *faces = advance(False, False, force, moved, traction1, pu, pv, inverse)
    gu1, left_seen = lax.optimization_barrier((gu1, faces[0]))
    gu2 = pl.pallas_call(
        functools.partial(third_interface, dims),
        out_shape=wide,
        in_specs=[vmem] * 4,
        out_specs=vmem,
        scratch_shapes=[held] * 2 + [place],
        name="interface2",
        cost_estimate=cost(4),
    )(gu1, gv1, ginv, traction1)
    moved, folded = exchange_lat(*exchange_lon(*faces[:2]), *faces[2:], gu2)
    xv2, folded = lax.optimization_barrier((xv2, folded))
    xv3, traction2, kept = pl.pallas_call(
        functools.partial(third_traction, dims),
        out_shape=(xvs, grid_rows, shaped(3, 3, nown, degrees)),
        in_specs=[vmem] * 11 + [smem],
        out_specs=(vmem,) * 3,
        scratch_shapes=[pltpu.VMEM((6, degrees, degrees), f32)] + hats,
        name="traction2",
        cost_estimate=cost(5),
    )(*tables, xv2, hist, gu2, coef1, coef0, owner_order)
    new_u, new_v = advance(False, True, force, moved, traction2, pu, pv, inverse)
    new_history = jnp.concatenate([kept, past[: lags - 1 - STEPS]], axis=0).transpose(2, 0, 1, 3)
    return (
        new_u.reshape(displacement.shape),
        new_v.reshape(velocity.shape),
        new_history,
        xv3[0:3, 0],
        xv3[3:6, 0],
    )


def solution(mesh):
    field = P(None, None, None, None, "blk", "lat", None)
    nodal = P(None, None, None, "blk", "lat", None)
    columns = P(("blk", "lat"), None, None, None)
    in_specs = (field, field, nodal, nodal, columns, P(), P(), P(), P())
    out_specs = (field, field, columns, P(), P())
    return jax.shard_map(
        functools.partial(on_device, (mesh.shape["blk"], mesh.shape["lat"])),
        mesh=mesh,
        in_specs=in_specs,
        out_specs=out_specs,
        check_vma=False,
    )
```

```python
import functools
import math

import jax
import jax.numpy as jnp
import numpy as np
from jax import lax
from jax.experimental import pallas as pl
from jax.experimental.pallas import tpu as pltpu
from jax.sharding import PartitionSpec as P

STEPS = 3
pole_gap = 0.1
time_step = 0.03
rigid_gain = 20.0
highest = lax.Precision.HIGHEST
f32 = jnp.float32
ROWS = 8
N3 = 125
HALF = 13
CHUNKS = 8
HEAD = 24
PAY = HEAD + 3 * CHUNKS


def node_tables():
    points = np.array([-1.0, -math.sqrt(3.0 / 7.0), 0.0, math.sqrt(3.0 / 7.0), 1.0])
    weights = np.array([0.1, 49.0 / 90.0, 32.0 / 45.0, 49.0 / 90.0, 0.1])
    products = np.array(
        [np.prod([points[i] - points[j] for j in range(5) if j != i]) for i in range(5)]
    )
    slopes = np.zeros((5, 5))
    for i in range(5):
        for j in range(5):
            if i == j:
                slopes[i, j] = sum(1.0 / (points[i] - points[n]) for n in range(5) if n != i)
            else:
                slopes[i, j] = products[i] / products[j] / (points[i] - points[j])
    return points, weights, slopes


POINTS, WEIGHTS, SLOPES = node_tables()
VOLUME = [
    float(WEIGHTS[a] * WEIGHTS[b] * WEIGHTS[c])
    for a in range(5)
    for b in range(5)
    for c in range(5)
]


def centro_apply(matrix, x):
    s0, s1, d0, d1 = x[0] + x[4], x[1] + x[3], x[0] - x[4], x[1] - x[3]
    even, odd = [], []
    for i in range(2):
        even.append(
            (0.5 * float(matrix[i][0] + matrix[i][4])) * s0
            + (0.5 * float(matrix[i][1] + matrix[i][3])) * s1
            + float(matrix[i][2]) * x[2]
        )
    for i in range(3):
        odd.append(
            (0.5 * float(matrix[i][0] - matrix[i][4])) * d0
            + (0.5 * float(matrix[i][1] - matrix[i][3])) * d1
        )
    return [odd[0] + even[0], odd[1] + even[1], odd[2], odd[1] - even[1], odd[0] - even[0]]


def row_ids(shape):
    return lax.broadcasted_iota(jnp.int32, shape, len(shape) - 2)


def lane_ids(shape):
    return lax.broadcasted_iota(jnp.int32, shape, len(shape) - 1)


def stiffness(u, scaled, out, aux, ny):
    lanes = u.shape[-1]
    rows = row_ids((ROWS, lanes))
    for node in range(N3):
        x = u[node]
        spread = jnp.where(
            rows < ny,
            pltpu.roll(x, ny, 0),
            jnp.where(rows < 2 * ny, pltpu.roll(x, 2 * ny, 0), pltpu.roll(x, 3 * ny, 0)),
        )
        scaled[node] = spread * (-VOLUME[node])
    for direction in range(3):
        stride = (25, 5, 1)[direction]

        def line(i, carry, direction=direction, stride=stride):
            if direction == 0:
                base = i
            elif direction == 1:
                base = (i // 5) * 25 + i % 5
            else:
                base = i * 5
            slope = centro_apply(SLOPES, [u[base + j * stride] for j in range(5)])
            flux = [slope[j] * scaled[base + j * stride] for j in range(5)]
            force = centro_apply(SLOPES.T, flux)
            for j in range(5):
                at = base + j * stride
                if direction == 0:
                    out[at] = force[j]
                else:
                    out[at] = out[at] + force[j]
            return carry

        lax.fori_loop(0, 25, line, 0, unroll=5)
    if aux is not None:
        for node in range(N3):
            out[node] = jnp.where(rows < 3 * ny, out[node], aux[node] * VOLUME[node])


def join_rows(out, ny):
    lanes = out.shape[-1]
    y = row_ids((ROWS, lanes)) % ny
    for a in range(5):
        for c in range(5):
            low, high = a * 25 + c, a * 25 + 20 + c
            first, last = out[low], out[high]
            out[high] = last + jnp.where(y < ny - 1, pltpu.roll(first, ROWS - 1, 0), 0.0)
            out[low] = first + jnp.where(y > 0, pltpu.roll(last, 1, 0), 0.0)


def join_radius(out):
    lanes = out.shape[-1]
    z = lane_ids((ROWS, lanes))
    for ab in range(25):
        low, high = ab * 5, ab * 5 + 4
        first, last = out[low], out[high]
        out[high] = last + jnp.where(z < lanes - 1, pltpu.roll(first, lanes - 1, 1), 0.0)
        out[low] = first + jnp.where(z > 0, pltpu.roll(last, 1, 1), 0.0)


def spread_inverse(x, ny):
    rows = row_ids(x.shape)
    inverse = 1.0 / jnp.where(rows < 3 * ny, 1.0, x)
    return jnp.where(
        rows < ny,
        pltpu.roll(inverse, ny, 0),
        jnp.where(rows < 2 * ny, pltpu.roll(inverse, 2 * ny, 0), pltpu.roll(inverse, 3 * ny, 0)),
    )


def pack(source, aux, out, ny):
    for node in range(N3):
        for k in range(3):
            out[node, k * ny : (k + 1) * ny, :] = source[k, node]
        out[node, 3 * ny : 4 * ny, :] = aux[node]


def gather_kernel(
    dims, u, v, rig, dens, hist, kern, up, down, diag, cosrow, owner, out, pu, pv, wide, turned
):
    ny, nlat, nown, rows_all, degrees = dims
    depth = u.shape[-1]
    out[...] = jnp.zeros(out.shape, f32)
    pack(u, rig, pu, ny)
    pack(v, dens, pv, ny)
    for ab in range(25):
        low, high = ab * 5, ab * 5 + 4
        above = pltpu.roll(pv[low], depth - 1, 1)
        pv[high] = pv[high] + jnp.where(row_ids((ROWS, depth)) >= 3 * ny, above, 0.0)
    lane = lane_ids((ROWS, depth))
    for n in range(16):
        merged = jnp.zeros((ROWS, depth), f32)
        for q in range(CHUNKS):
            if q * 16 + n < N3:
                x = pu[q * 16 + n]
                merged = jnp.where(lane // 2 == q, pltpu.roll(x, 2 * q, 1) if q else x, merged)
                at = 2 * CHUNKS + q
                merged = jnp.where(lane == at, pltpu.roll(pv[q * 16 + n], at, 1), merged)
        turned[n * ROWS : (n + 1) * ROWS, :] = merged
    out[HEAD:PAY, :] = turned[...].T[0 : PAY - HEAD]
    lags = kern.shape[2]
    accs = [jnp.zeros((nown, degrees), f32) for _ in range(9)]
    for lag in range(1, lags):
        for k in range(3):
            for m in range(3):
                weight = kern[k, m, lag : lag + 1, :]
                for n in range(3):
                    if lag - n - 1 >= 0:
                        accs[n * 3 + k] = accs[n * 3 + k] + weight * hist[lag - n - 1, m]
    held = accs
    if nown < ROWS:
        pad = jnp.zeros((ROWS - nown, degrees), f32)
        held = [jnp.concatenate([x, pad], axis=0) for x in accs]
    device = lax.axis_index("blk") * nlat + lax.axis_index("lat")
    width = rows_all
    across = max(degrees, width)
    rows = row_ids((ROWS, across))
    order = jnp.zeros((ROWS, across), jnp.int32)
    for j in range(nown):
        order = jnp.where(rows == j, lax.rem(owner[device * nown + j], degrees), order)
    hot = jnp.where(order[:, 0:degrees] == lane_ids((ROWS, degrees)), 1.0, 0.0)
    contract = (((1,), (1,)), ((), ()))
    up_own = lax.dot_general(hot, up[...], contract, precision=highest, preferred_element_type=f32)
    down_own = lax.dot_general(
        hot, down[...], contract, precision=highest, preferred_element_type=f32
    )
    start = lax.dot_general(hot, diag[...], contract, precision=highest, preferred_element_type=f32)
    cosine = jnp.broadcast_to(cosrow[0:1, :], (ROWS, width))
    comp = (lane_ids((ROWS, width)) % (3 * ny)) // ny
    which = order[:, 0:width]
    prev = jnp.zeros((ROWS, width), f32)
    before = jnp.zeros((ROWS, width), f32)
    sums = [jnp.zeros((ROWS, width), f32) for _ in range(3)]
    for level in range(degrees):
        value = up_own[:, level : level + 1] * (
            cosine * prev - down_own[:, level : level + 1] * before
        )
        value = jnp.where(which == level, start, value)
        for n in range(3):
            h = jnp.where(
                comp == 0,
                held[n * 3][:, level : level + 1],
                jnp.where(
                    comp == 1,
                    held[n * 3 + 1][:, level : level + 1],
                    held[n * 3 + 2][:, level : level + 1],
                ),
            )
            sums[n] = sums[n] + h * value
        before, prev = prev, value
    wide[...] = jnp.zeros(wide.shape, f32)
    for n in range(3):
        wide[:, n * width : (n + 1) * width] = sums[n]
    for q in range(HEAD // ROWS):
        out[q * ROWS : (q + 1) * ROWS, :] = wide[:, q * 128 : (q + 1) * 128]


def write_faces(force, left, right, low, high):
    for b in range(5):
        for c in range(5):
            left[b * 5 + c] = force[b * 5 + c]
            right[b * 5 + c] = force[100 + b * 5 + c]
    for a in range(5):
        for c in range(5):
            low[a * 5 + c] = force[a * 25 + c]
            high[a * 5 + c] = force[a * 25 + 20 + c]


def start_kernel(ny, u, v, rig, dens, pu, pv, force, left, right, low, high, scaled):
    pack(u, rig, pu, ny)
    pack(v, dens, pv, ny)
    stiffness(pu, scaled, force, pv, ny)
    join_rows(force, ny)
    join_radius(force)
    write_faces(force, left, right, low, high)


def fold_kernel(ny, from_left, from_right, low, high, token, out_low, out_high):
    y = row_ids(low.shape[1:]) % ny

    def full(ref, n, at):
        if n < 5:
            return ref[n] + from_left[at + n]
        return ref[n] + from_right[at + n - 20] if n >= 20 else ref[n]

    for p in range(HALF):
        first, second = full(low, p, 0), full(high, p, 20)
        if p + HALF < 25:
            first = jnp.where(y == 0, first, pltpu.roll(full(low, p + HALF, 0), 1, 0))
            second = jnp.where(y > 0, second, pltpu.roll(full(high, p + HALF, 20), ROWS - 1, 0))
        out_low[p] = first
        out_high[p] = second


def advance_kernel(dims, first, last, *refs):
    ny, nlat, lanes = dims
    refs = list(refs)
    force, from_left, from_right, from_low, from_high, traction, pu, pv = refs[:8]
    refs = refs[8:]
    if not first:
        inverse = refs.pop(0)
    if last:
        out_u, out_v, total = refs
    else:
        new_u, new_v, new_force, left, right, low, high = refs[:7]
        refs = refs[7:]
        if first:
            inverse = refs.pop(0)
        total, scaled = refs
    lat = lax.axis_index("lat")
    rows = row_ids((ROWS, lanes))
    y = rows % ny
    z = lane_ids((ROWS, lanes))
    for node in range(N3):
        total[node] = force[node]
    for bc in range(25):
        total[bc] = total[bc] + from_left[bc]
        total[100 + bc] = total[100 + bc] + from_right[bc]
    has_low = jnp.where(lat > 0, 1, 0)
    has_high = jnp.where(lat < nlat - 1, 1, 0)
    take_low = jnp.logical_and(y == 0, jnp.full(y.shape, has_low, jnp.int32) > 0)
    take_high = jnp.logical_and(y == ny - 1, jnp.full(y.shape, has_high, jnp.int32) > 0)
    for a in range(5):
        for c in range(5):
            at = a * 25 + c
            n = a * 5 + c
            if n < HALF:
                lower = pltpu.roll(from_low[n], ROWS - 1, 0)
                upper = pltpu.roll(from_high[n], 1, 0)
            else:
                lower, upper = from_low[n - HALF], from_high[n - HALF]
            total[at] = total[at] + jnp.where(take_low, lower, 0.0)
            total[at + 20] = total[at + 20] + jnp.where(take_high, upper, 0.0)
    if first:
        for node in range(N3):
            inverse[node] = spread_inverse(total[node], ny)
    for a in range(5):
        wa = float(WEIGHTS[a] * (2.0 if a in (0, 4) else 1.0))
        for b in range(5):
            tr = traction[b * ROWS : (b + 1) * ROWS, :]
            if tr.shape[1] != lanes:
                tr = tr[:, 0:lanes]
            moved = pltpu.roll(tr, lanes - a, 1) if a else tr
            at = a * 25 + b * 5
            total[at] = total[at] - (wa * pick_face(b, rows, ny, has_low, has_high)) * jnp.where(
                z == 0, moved, 0.0
            )
    for node in range(N3):
        speed = pv[node] + time_step * total[node] * inverse[node]
        place = pu[node] + time_step * speed
        if last:
            for k in range(3):
                out_v[k, node] = speed[k * ny : (k + 1) * ny, :]
                out_u[k, node] = place[k * ny : (k + 1) * ny, :]
        else:
            new_v[node] = speed
            new_u[node] = jnp.where(rows < 3 * ny, place, pu[node])
    if not last:
        stiffness(new_u, scaled, new_force, None, ny)
        join_rows(new_force, ny)
        join_radius(new_force)
        write_faces(new_force, left, right, low, high)


def pick_face(b, rows, ny, has_low, has_high):
    weight = float(WEIGHTS[b])
    y = rows % ny
    if b == 0:
        shared = jnp.logical_or(y > 0, jnp.full(y.shape, has_low, jnp.int32) > 0)
    elif b == 4:
        shared = jnp.logical_or(y < ny - 1, jnp.full(y.shape, has_high, jnp.int32) > 0)
    else:
        return weight
    return jnp.where(shared, 2.0 * weight, weight)


def unpack(pieces, part, rows_ref, out, dims):
    ny, nlat, nblk, lanes = dims
    count = nblk * nlat
    rows_ref[...] = jnp.zeros(rows_ref.shape, f32)
    for q in range(CHUNKS):
        for core, ref in enumerate(pieces):
            n = ref.shape[0] // PAY
            for ez in range(2 if part == 0 else 1):
                at = HEAD + 2 * q + ez if part == 0 else HEAD + 2 * CHUNKS + q
                rows_ref[q, pl.ds(ez * count + core, n, stride=2), :] = ref[
                    pl.ds(at, n, stride=PAY), :
                ]
    for q in range(CHUNKS):
        nodes = min(16, N3 - q * 16)
        for strip in range(lanes // 128):
            block = rows_ref[q, strip * 128 : (strip + 1) * 128, :].T
            out[q * 16 : q * 16 + nodes, :, strip * 128 : (strip + 1) * 128] = block[
                : nodes * ROWS
            ].reshape(nodes, ROWS, 128)


def split3(x):
    hi = x.astype(jnp.bfloat16)
    rest = x - hi.astype(f32)
    mid = rest.astype(jnp.bfloat16)
    low = (rest - mid.astype(f32)).astype(jnp.bfloat16)
    return hi, mid, low


def place_matrices(out, dims, fs):
    ny, nlat, nblk, lanes = dims
    lam = row_ids((lanes, fs))
    offset = lane_ids((lanes, fs)) - lax.div(lam, nlat) * 5
    for i in range(nlat):
        mine = jnp.logical_and(lax.rem(lam, nlat) == i, lam < nlat * nblk)
        at = jnp.where(mine, offset, -1)
        for a in range(5):
            out[a * lanes : (a + 1) * lanes, i * fs : (i + 1) * fs] = jnp.where(
                at == a, 1.0, 0.0
            ).astype(jnp.bfloat16)


def times_onehot(x, place, transposed):
    n = x.shape[0]
    parts = jnp.concatenate(split3(x), axis=0)
    axes = (((1,), (1 if transposed else 0,)), ((), ()))
    y = lax.dot_general(parts, place[...], axes, preferred_element_type=f32)
    return y[0:n] + y[n : 2 * n] + y[2 * n : 3 * n]


def lat_of(i, nlat):
    return lax.bitwise_xor(lax.axis_index("lat"), jnp.int32(i))


def to_traction(dims, n, u, tables, scratch, xv, hist, coef_refs, coef_out, xv_out, out):
    ny, nlat, nblk, lanes = dims
    legendre, circle, rowc, lanec, weights, kernels = tables
    state, hat, shat, mix, place, kern = scratch
    kern[...] = jnp.zeros(kern.shape, f32)
    for s in range(1 + len(coef_refs)):
        for k in range(3):
            for m in range(3):
                at = (s * 3 + k) * 3 + m
                kern[at : at + 1, :] = kernels[k, m, s : s + 1, :]
    kern[...] = kern[...].T
    degrees = legendre.shape[-1]
    fs = circle.shape[0]
    grid = times_onehot(
        jnp.concatenate(
            [
                jnp.concatenate([u[a * 25 + b * 5] for b in range(5)], axis=0)
                for a in range(5)
            ],
            axis=1,
        ),
        place,
        False,
    )
    cosphi, sinphi, wphi = lanec[0:1, :], lanec[1:2, :], weights[0:1, :]
    x0, x1, x2 = xv[0:1, 0:1], xv[1:2, 0:1], xv[2:3, 0:1]
    along = x0 * cosphi + x1 * sinphi
    across = x1 * cosphi - x0 * sinphi
    fields, columns = [], []
    for i in range(nlat):
        here = rowc[pl.ds(pl.multiple_of(lat_of(i, nlat) * (5 * ROWS), ROWS), 5 * ROWS), :]
        columns.append(here)
        ca, cc, cz, at = (here[:, j : j + 1] for j in range(4))
        rigid = ca * along + cc * across + cz * x2
        fields.append((grid[:, i * fs : (i + 1) * fs] - rigid) * at * wphi)
    hat[...] = jnp.dot(
        jnp.concatenate(fields, axis=0),
        circle[...],
        precision=highest,
        preferred_element_type=f32,
    )
    blocks = degrees // ROWS
    zero = jnp.zeros((ROWS, degrees), f32)
    ids = row_ids((ROWS, degrees))
    even = (ids + lane_ids((ROWS, degrees))) % 2 == 0
    lat = lax.axis_index("lat")
    spots = nlat // 2 * 5 * ny

    def block_starts(at, b):
        north = lax.bitwise_xor(jnp.int32(at), lat)
        south = lax.bitwise_xor(jnp.int32(nlat - 1 - at), lat)
        return (
            pl.multiple_of((north * 5 + b) * ROWS, ROWS),
            pl.multiple_of((south * 5 + 4 - b) * ROWS, ROWS),
        )

    for at in range(nlat // 2):
        for b in range(5):
            north, south = block_starts(at, b)
            for part in range(2):
                sl = slice(part * degrees, (part + 1) * degrees)
                upper, lower = hat[pl.ds(north, ROWS), sl], hat[pl.ds(south, ROWS), sl]
                lower = jnp.where(
                    ids % ny == 0, pltpu.roll(lower, ROWS - 1, 0), pltpu.roll(lower, 1, 0)
                )
                both, apart = upper + lower, upper - lower
                for k in range(3):
                    for y in range(ny):
                        r = k * ny + y
                        mix[((at * 5 + b) * ny + y) * 6 + k * 2 + part] = jnp.where(
                            even, both[r : r + 1], apart[r : r + 1]
                        )
    group = 4

    def analyse(blk, carry):
        l0 = pl.multiple_of(blk * (group * ROWS), group * ROWS)
        accs = [[zero] * 6 for _ in range(group)]
        for spot in range(spots):
            values = [mix[spot * 6 + kp] for kp in range(6)]
            for h in range(group):
                p = legendre[spot, pl.ds(l0 + h * ROWS, ROWS), :]
                for kp in range(6):
                    accs[h][kp] = accs[h][kp] + p * values[kp]
        for h in range(group):
            sl = pl.ds(l0 + h * ROWS, ROWS)
            for kp in range(6):
                coef_out[kp, sl, :] = accs[h][kp]
            for k in range(3):
                totals = [zero, zero]
                for s, ref in enumerate([None] + coef_refs):
                    for m in range(3):
                        col = (s * 3 + k) * 3 + m
                        weight = jnp.broadcast_to(kern[sl, col : col + 1], (ROWS, degrees))
                        for part in range(2):
                            kp = m * 2 + part
                            value = accs[h][kp] if s == 0 else ref[kp, sl, :]
                            totals[part] = totals[part] + weight * value
                for part in range(2):
                    state[k * 2 + part, sl, :] = totals[part]
        return carry

    lax.fori_loop(0, blocks // group, analyse, 0)

    def synth(nb, carry):
        at, b = lax.div(nb, 5), lax.rem(nb, 5)
        accs = [[zero] * 6 for _ in range(ny)]
        for blk in range(blocks):
            sl = slice(blk * ROWS, (blk + 1) * ROWS)
            held = [state[kp, sl, :] for kp in range(6)]
            for y in range(ny):
                p = legendre[nb * ny + y, sl, :]
                for kp in range(6):
                    accs[y][kp] = accs[y][kp] + p * held[kp]
        north, south = block_starts(at, b)
        for part in range(2):
            upper = lower = zero
            for k in range(3):
                for y in range(ny):
                    acc = accs[y][k * 2 + part]
                    total = jnp.sum(acc, axis=0, keepdims=True)
                    signed = jnp.sum(jnp.where(even, acc, -acc), axis=0, keepdims=True)
                    upper = jnp.where(ids == k * ny + y, total, upper)
                    lower = jnp.where(ids == k * ny + ny - 1 - y, signed, lower)
            sl = slice(part * degrees, (part + 1) * degrees)
            shat[pl.ds(north, ROWS), sl] = upper
            shat[pl.ds(south, ROWS), sl] = lower
        return carry

    lax.fori_loop(0, nlat // 2 * 5, synth, 0)
    traction = lax.dot_general(
        shat[...],
        circle[...],
        (((1,), (1,)), ((), ())),
        precision=highest,
        preferred_element_type=f32,
    )
    count = nlat * 5 * ROWS
    earlier = [
        hist[pl.ds(pl.multiple_of(n * count + lat_of(i, nlat) * (5 * ROWS), ROWS), 5 * ROWS), :]
        for i in range(nlat)
    ]
    traction = traction + jnp.concatenate(earlier, axis=0)
    out[...] = traction
    here = jnp.concatenate(columns, axis=0)
    ca, cc, cz, at = (here[:, j : j + 1] for j in range(4))
    weighted = traction * at * wphi
    radial = jnp.sum(weighted * ca, axis=0, keepdims=True)
    turning = jnp.sum(weighted * cc, axis=0, keepdims=True)
    polar = jnp.sum(weighted * cz, axis=0, keepdims=True)
    pulls = [
        jnp.sum(radial * cosphi - turning * sinphi, axis=1, keepdims=True),
        jnp.sum(radial * sinphi + turning * cosphi, axis=1, keepdims=True),
        jnp.sum(polar, axis=1, keepdims=True),
    ]
    for j in range(3):
        speed = xv[3 + j : 4 + j, :] + time_step * rigid_gain * pulls[j]
        xv_out[3 + j : 4 + j, :] = speed
        xv_out[j : j + 1, :] = xv[j : j + 1, :] + time_step * speed
    xv_out[6:8, :] = jnp.zeros((2, xv_out.shape[1]), f32)


def first_interface(dims, npieces, *refs):
    ny, nlat, nblk, lanes = dims
    pieces = refs[:npieces]
    tables, order_circle, xv = refs[npieces : npieces + 6], refs[npieces + 6], refs[npieces + 7 : npieces + 9]
    u, hist, coef, xv_out, out = refs[npieces + 9 : npieces + 14]
    rows_ref, held, start, *scratch = refs[npieces + 14 :]
    for j in range(3):
        start[j : j + 1, :] = jnp.full((1, start.shape[1]), xv[0][j], f32)
        start[3 + j : 4 + j, :] = jnp.full((1, start.shape[1]), xv[1][j], f32)
    place_matrices(scratch[4], dims, tables[1].shape[0])
    unpack(pieces, 0, rows_ref, u, dims)
    for core, ref in enumerate(pieces):
        for d in range(ref.shape[0] // PAY):
            at = (2 * d + core) * ROWS
            for q in range(HEAD // ROWS):
                held[at : at + ROWS, q * 128 : (q + 1) * 128] = ref[
                    d * PAY + q * ROWS : d * PAY + (q + 1) * ROWS, :
                ]
    group = 3 * ny
    groups = hist.shape[0] // ROWS
    summed = lax.dot_general(
        held[...],
        order_circle[...],
        (((0,), (0,)), ((), ())),
        precision=highest,
        preferred_element_type=f32,
    )
    spare = jnp.zeros((ROWS - group, summed.shape[1]), f32)
    for g in range(groups):
        hist[g * ROWS : (g + 1) * ROWS, :] = jnp.concatenate(
            [summed[g * group : (g + 1) * group], spare], axis=0
        )
    to_traction(dims, 0, u, tables, scratch, start, hist, [], coef, xv_out, out)


def interface_force(dims, u, aux, scaled, force):
    ny, nlat, nblk, lanes = dims
    count = nlat * nblk
    stiffness(u, scaled, force, aux, ny)
    join_rows(force, ny)
    shape = (ROWS, lanes)
    lam = lane_ids(shape)
    rows = row_ids(shape)
    y = rows % ny
    lat_at = lax.rem(lam, nlat)
    blk_at = lax.rem(lax.div(lam, nlat), nblk)
    for ab in range(25):
        high = ab * 5 + 4
        force[high] = force[high] + jnp.where(
            lam < count, pltpu.roll(force[ab * 5], lanes - count, 1), 0.0
        )
    wrap = count - nlat
    for bc in range(25):
        first, last = force[bc], force[100 + bc]
        lower = jnp.where(
            blk_at == 0, pltpu.roll(last, lanes - wrap, 1), pltpu.roll(last, nlat, 1)
        )
        upper = jnp.where(
            blk_at == nblk - 1, pltpu.roll(first, wrap, 1), pltpu.roll(first, lanes - nlat, 1)
        )
        force[bc] = first + lower
        force[100 + bc] = last + upper
    absolute = lax.bitwise_xor(lat_at, jnp.full(shape, lax.axis_index("lat"), jnp.int32))
    take_low = jnp.logical_and(y == 0, absolute > 0)
    take_high = jnp.logical_and(y == ny - 1, absolute < nlat - 1)

    def neighbour(x, by_one):
        back, ahead = pltpu.roll(x, 1, 1), pltpu.roll(x, lanes - 1, 1)
        far = jnp.where(lat_at == 0, pltpu.roll(x, lanes - 3, 1), pltpu.roll(x, 3, 1))
        middle = jnp.logical_or(lat_at == 1, lat_at == 2)
        one = jnp.where(lat_at % 2 == 0, ahead, back)
        three = jnp.where(middle, jnp.where(lat_at == 1, ahead, back), far)
        return jnp.where(by_one, one, three)

    for a in range(5):
        for c in range(5):
            low, high = a * 25 + c, a * 25 + 20 + c
            first, last = force[low], force[high]
            lower = neighbour(last, absolute % 2 == 1)
            upper = neighbour(first, absolute % 2 == 0)
            force[low] = first + jnp.where(
                take_low, pltpu.roll(lower, ROWS - (ny - 1), 0), 0.0
            )
            force[high] = last + jnp.where(take_high, pltpu.roll(upper, ny - 1, 0), 0.0)


def add_traction(dims, traction, force, place):
    ny, nlat, nblk, lanes = dims
    shape = (ROWS, lanes)
    lam = lane_ids(shape)
    rows = row_ids(shape)
    absolute = lax.bitwise_xor(lax.rem(lam, nlat), jnp.full(shape, lax.axis_index("lat"), jnp.int32))
    y = rows % ny
    grid = jnp.concatenate(
        [traction[i * 5 * ROWS : (i + 1) * 5 * ROWS, :] for i in range(nlat)], axis=1
    )
    spread = times_onehot(grid, place, True)
    for a in range(5):
        moved = spread[:, a * lanes : (a + 1) * lanes]
        wa = float(WEIGHTS[a] * (2.0 if a in (0, 4) else 1.0))
        for b in range(5):
            weight = float(WEIGHTS[b]) * wa
            if b == 0:
                shared = jnp.logical_or(y > 0, absolute > 0)
            elif b == 4:
                shared = jnp.logical_or(y < ny - 1, absolute < nlat - 1)
            else:
                shared = None
            face = weight if shared is None else jnp.where(shared, 2.0 * weight, weight)
            at = a * 25 + b * 5
            force[at] = force[at] - face * moved[b * ROWS : (b + 1) * ROWS]


def second_interface(dims, npieces, *refs):
    ny, nlat, nblk, lanes = dims
    pieces = refs[:npieces]
    u, traction, new_u, new_v, inverse, rows_ref, force, scaled, v, place = refs[npieces:]
    place_matrices(place, dims, traction.shape[1])
    unpack(pieces, 1, rows_ref, v, dims)
    interface_force(dims, u, v, scaled, force)
    rows = row_ids((ROWS, lanes))
    lam = lane_ids((ROWS, lanes))
    for node in range(N3):
        mass = force[node]
        inverse[node] = spread_inverse(jnp.where(lam < nlat * nblk, mass, 1.0), ny)
    add_traction(dims, traction, force, place)
    for node in range(N3):
        speed = v[node] + time_step * force[node] * inverse[node]
        new_v[node] = speed
        new_u[node] = jnp.where(rows < 3 * ny, u[node] + time_step * speed, u[node])


def second_traction(dims, *refs):
    tables, (xv, hist, u, coef0) = refs[:6], refs[6:10]
    coef, xv_out, out, *scratch = refs[10:]
    place_matrices(scratch[4], dims, tables[1].shape[0])
    to_traction(dims, 1, u, tables, scratch, xv, hist, [coef0], coef, xv_out, out)


def third_interface(dims, u, v, inverse, traction, new_u, force, scaled, place):
    place_matrices(place, dims, traction.shape[1])
    interface_force(dims, u, None, scaled, force)
    add_traction(dims, traction, force, place)
    for ab in range(25):
        node = ab * 5
        speed = v[node] + time_step * force[node] * inverse[node]
        new_u[node] = u[node] + time_step * speed


def third_traction(dims, *refs):
    ny, nlat, nblk, lanes = dims
    tables, (xv, hist, u, coef1, coef0, owner) = refs[:6], refs[6:12]
    xv_out, out, kept, coef, *scratch = refs[12:]
    place_matrices(scratch[4], dims, tables[1].shape[0])
    to_traction(dims, 2, u, tables, scratch, xv, hist, [coef1, coef0], coef, xv_out, out)
    nown = kept.shape[2]
    degrees = tables[0].shape[-1]
    device = lax.axis_index("blk") * nlat + lax.axis_index("lat")
    ids = row_ids((ROWS, 2 * degrees))
    column = jnp.full((ROWS, 2 * degrees), -1, jnp.int32)
    for j in range(nown):
        column = jnp.where(ids == j, owner[device * nown + j], column)
    hot = jnp.where(column == lane_ids((ROWS, 2 * degrees)), 1.0, 0.0)
    for n, ref in enumerate((coef, coef1, coef0)):
        for k in range(3):
            both = jnp.concatenate([ref[2 * k], ref[2 * k + 1]], axis=1)
            mine = lax.dot_general(
                hot, both, (((1,), (1,)), ((), ())), precision=highest, preferred_element_type=f32
            )
            kept[n, k] = mine[0:nown]


def legendre_tables(colatitude, degrees):
    cosine = np.cos(colatitude)[:, None]
    sine = np.sin(colatitude)[:, None]
    orders = np.arange(degrees, dtype=np.float64)[None, :]
    factor = np.where(
        orders == 0,
        math.sqrt(0.5),
        -np.sqrt((2.0 * orders + 1.0) / np.maximum(2.0 * orders, 1.0)) * sine,
    )
    diagonal = np.cumprod(factor, axis=1)
    levels = np.zeros((len(colatitude), degrees, degrees))
    ups = np.zeros((degrees, degrees))
    downs = np.zeros((degrees, degrees))
    previous = before = np.zeros((len(colatitude), degrees))
    for level in range(degrees):
        above = orders < level
        up = np.where(
            above,
            np.sqrt(
                max(4.0 * level * level - 1.0, 0.0) / np.maximum(level * level - orders**2, 1.0)
            ),
            0.0,
        )
        lowered = (level - 1.0) ** 2
        down = np.where(
            above,
            np.sqrt(np.maximum(lowered - orders**2, 0.0) / max(4.0 * lowered - 1.0, 1.0)),
            0.0,
        )
        values = up * (cosine * previous - down * before)
        values = np.where(orders == level, diagonal, values)
        levels[:, level, :] = values
        ups[level], downs[level] = up[0], down[0]
        before, previous = previous, values
    return (
        levels.astype(np.float32),
        ups.astype(np.float32),
        downs.astype(np.float32),
        diagonal.astype(np.float32),
    )


def on_device(
    mesh_sizes,
    displacement,
    velocity,
    rigidity,
    density,
    history,
    kernel,
    owner_order,
    rigid_offset,
    rigid_velocity,
):
    nblk, nlat = mesh_sizes
    nx, ny, depth = displacement.shape[4:]
    degrees = kernel.shape[3]
    lags = kernel.shape[0]
    nown = history.shape[0]
    lat_elems, lon_elems = ny * nlat, nblk
    nt, nf = 5 * lat_elems, 5 * lon_elems
    count = nblk * nlat
    lanes = -(-2 * count // 128) * 128
    fs = -(-nf // 128) * 128
    rows_all = nlat * 5 * ROWS
    hist_rows = nlat * 5 * 3 * ny
    assert nx == 1 and 4 * ny == ROWS and nlat == 4 and 3 * hist_rows <= 16 * HEAD
    dims = (ny, nlat, nblk, lanes)
    blk, lat = lax.axis_index("blk"), lax.axis_index("lat")

    theta_step = (math.pi - 2.0 * pole_gap) / lat_elems
    phi_step = 2.0 * math.pi / lon_elems
    theta = pole_gap + (np.arange(nt) // 5 + 0.5 * (1.0 + np.tile(POINTS, lat_elems))) * theta_step
    phi = (np.arange(nf) // 5 + 0.5 * (1.0 + np.tile(POINTS, lon_elems))) * phi_step
    table, ups, downs, diagonal = legendre_tables(theta, degrees)
    orders = np.arange(degrees)[None, :]
    angles = phi[:, None] * orders
    cosines = np.where(orders == 0, 1.0 / math.sqrt(2.0 * math.pi), np.cos(angles) / math.sqrt(math.pi))
    sines = np.where(orders == 0, 0.0, np.sin(angles) / math.sqrt(math.pi))
    circle_all = np.concatenate([cosines, sines], axis=1).astype(np.float32)
    r = np.arange(rows_all)
    r_lat, r_b, r_s = r // (5 * ROWS), (r // ROWS) % 5, r % ROWS
    r_k, r_y = r_s // ny, r_s % ny
    r_t = (r_lat * ny + r_y) * 5 + r_b
    real = r_k < 3
    th = theta[r_t]
    rowc_all = np.zeros((rows_all, 8))
    rowc_all[:, 0] = np.where(r_k == 0, np.sin(th), np.where(r_k == 1, np.cos(th), 0.0))
    rowc_all[:, 1] = np.where(r_k == 2, 1.0, 0.0)
    rowc_all[:, 2] = np.where(r_k == 0, np.cos(th), np.where(r_k == 1, -np.sin(th), 0.0))
    rowc_all[:, 3] = np.where(
        real, 0.25 * theta_step * phi_step * WEIGHTS[r_b] * np.sin(th), 0.0
    )
    lanec_all = np.zeros((8, nf))
    lanec_all[0], lanec_all[1] = np.cos(phi), np.sin(phi)
    lanec_all[2] = np.tile(WEIGHTS, lon_elems)
    diag_rows = diagonal[r_t[real]]
    cos_rows = np.cos(th[real]).astype(np.float32)

    spot = np.arange(nt // 2)
    spot_t = (spot // (5 * ny) * ny + spot % ny) * 5 + spot // ny % 5
    north = jnp.asarray(table[spot_t])
    vmem = pl.BlockSpec(memory_space=pltpu.VMEM)
    smem = pl.BlockSpec(memory_space=pltpu.SMEM)
    def shaped(*dims_):
        return jax.ShapeDtypeStruct(dims_, f32)

    def local(*dims_):
        return pltpu.VMEM(dims_, f32) if lanes == 128 else shaped(*dims_)

    resident = lanes == 128
    limits = pltpu.CompilerParams(vmem_limit_bytes=24 * 1024 * 1024) if resident else None

    def remote(x):
        return pltpu.with_memory_space_constraint(x, pltpu.HBM)

    def near(x):
        return pltpu.with_memory_space_constraint(x, pltpu.VMEM)

    def call(kernel_fn, far=(), **kw):
        inner = pl.pallas_call(
            kernel_fn,
            compiler_params=limits,
            **kw,
        )
        specs = kw["in_specs"]

        def run(*xs):
            keep = [
                x if specs[i] is not vmem or not resident else remote(x) if i in far else near(x)
                for i, x in enumerate(xs)
            ]
            return inner(*keep)

        return run

    def cost(micros):
        return pl.CostEstimate(
            flops=int(micros * 5e6), transcendentals=0, bytes_accessed=int(micros * 1e6)
        )

    u4 = displacement.reshape(3, N3, ny, depth)
    v4 = velocity.reshape(3, N3, ny, depth)
    rig = rigidity.reshape(N3, ny, depth)
    dens = density.reshape(N3, ny, depth)
    past = history.transpose(1, 2, 0, 3)

    payload = call(
        functools.partial(gather_kernel, (ny, nlat, nown, hist_rows, degrees)),
        far=range(10),
        out_shape=local(PAY, 128),
        in_specs=[vmem] * 10 + [smem],
        out_specs=vmem,
        scratch_shapes=[pltpu.VMEM((N3, ROWS, depth), f32)] * 2
        + [pltpu.VMEM((ROWS, 16 * HEAD), f32), pltpu.VMEM((16 * ROWS, depth), f32)],
        name="gather",
        cost_estimate=cost(6),
    )(
        u4,
        v4,
        rig,
        dens,
        past,
        kernel.transpose(1, 2, 0, 3),
        jnp.asarray(ups),
        jnp.asarray(downs),
        jnp.asarray(diag_rows),
        jnp.asarray(np.tile(cos_rows[None], (8, 1))),
        owner_order,
    )

    def shifted(x, axis, size, by):
        return lax.ppermute(x, axis, [(s, (s - by) % size) for s in range(size)])

    def swapped(x, bit):
        return lax.ppermute(x, "lat", [(i, i ^ bit) for i in range(nlat)])

    column = jnp.concatenate([payload, swapped(payload, 2)], axis=0)
    if nblk <= 8:
        mine = [column] + [shifted(column, "blk", nblk, i) for i in range(1, nblk)]
        mine = jnp.concatenate(mine, axis=0)
        base_blk = blk
    else:
        mine = lax.all_gather(column, "blk", axis=0, tiled=True)
        base_blk = blk * 0
    packed = local(N3, ROWS, depth)
    face = local(25, ROWS, depth)
    buffer = pltpu.VMEM((N3, ROWS, depth), f32)
    pu, pv, force, *faces = call(
        functools.partial(start_kernel, ny),
        far=range(4),
        out_shape=(packed,) * 3 + (face,) * 4,
        in_specs=[vmem] * 4,
        out_specs=(vmem,) * 7,
        scratch_shapes=[buffer],
        name="forces",
        cost_estimate=cost(4),
    )(u4, v4, rig, dens)
    *faces, column_seen = lax.optimization_barrier((*faces, column))

    def exchange_lon(left, right):
        return shifted(right, "blk", nblk, -1), shifted(left, "blk", nblk, 1)

    def exchange_lat(from_left, from_right, low, high, token):
        half = local(HALF, ROWS, depth)
        low, high = call(
            functools.partial(fold_kernel, ny),
            out_shape=(half,) * 2,
            in_specs=[vmem] * 4 + [pl.BlockSpec(memory_space=pl.ANY)],
            out_specs=(vmem,) * 2,
            name="fold",
            cost_estimate=cost(1),
        )(from_left, from_right, low, high, token)
        received = shifted(high, "lat", nlat, -1), shifted(low, "lat", nlat, 1)
        return (from_left, from_right, *received), low


    def turned(values, axis):
        reach = np.take(values, np.arange(nf + fs) % nf, axis=axis).astype(np.float32)
        return lax.dynamic_slice_in_dim(jnp.asarray(reach), base_blk * 5, fs, axis)

    circle = turned(circle_all, 0)
    lanec = turned(lanec_all, 1)
    wphi = np.zeros((8, fs), np.float32)
    wphi[0, :nf] = np.tile(WEIGHTS, lon_elems)
    rowc = jnp.asarray(rowc_all.astype(np.float32))
    owners = owner_order.reshape(nblk, nlat, nown)
    owners = lax.dynamic_slice_in_dim(jnp.concatenate([owners, owners], 0), base_blk, nblk, 0)
    owners = jnp.take(owners, lax.bitwise_xor(lat, jnp.arange(nlat, dtype=jnp.int32)), axis=1)
    owners = jnp.pad(owners.reshape(count, nown), ((0, 0), (0, ROWS - nown)), constant_values=-1)
    owners = owners.reshape(count * ROWS)
    hot = (owners[:, None] == jnp.arange(2 * degrees, dtype=jnp.int32)[None, :]).astype(f32)
    order_circle = jnp.einsum("pc,fc->pf", hot, circle, precision=highest)
    tables = (north, circle, rowc, lanec, jnp.asarray(wphi), kernel.transpose(1, 2, 0, 3))

    wide = local(N3, ROWS, lanes)
    held = pltpu.VMEM((N3, ROWS, lanes), f32)
    coefs = local(6, degrees, degrees)
    grid_rows = local(rows_all, fs)
    hats = [
        pltpu.VMEM((6, degrees, degrees), f32),
        pltpu.VMEM((rows_all, 2 * degrees), f32),
        pltpu.VMEM((rows_all, 2 * degrees), f32),
        pltpu.VMEM((nlat // 2 * 5 * ny * 6, ROWS, degrees), f32),
        pltpu.VMEM((5 * lanes, nlat * fs), jnp.bfloat16),
        pltpu.VMEM((degrees, 128), f32),
    ]
    npieces = 2
    xvs = local(8, 128)
    *lon, mine, circle, lanec, order_circle = lax.optimization_barrier(
        (*exchange_lon(*faces[:2]), mine, circle, lanec, order_circle)
    )
    tables = (north, circle, rowc, lanec, jnp.asarray(wphi), kernel.transpose(1, 2, 0, 3))
    pieces = [mine, swapped(mine, 1)]
    moved, folded = exchange_lat(*lon, *faces[2:], column_seen)
    first_offset, folded = lax.optimization_barrier((rigid_offset, folded))
    gu, hist, coef0, xv1, traction0 = call(
        functools.partial(first_interface, dims, npieces),
        out_shape=(wide, local(3 * rows_all, fs), coefs, xvs, grid_rows),
        in_specs=[vmem] * (npieces + 7) + [smem] * 2,
        out_specs=(vmem,) * 5,
        scratch_shapes=[pltpu.VMEM((CHUNKS, lanes, 128), f32), pltpu.VMEM((count * ROWS, 16 * HEAD), f32)]
        + [pltpu.VMEM((8, 128), f32)]
        + hats,
        name="interface0",
        cost_estimate=cost(8),
    )(*pieces, *tables, order_circle, first_offset, rigid_velocity)

    def own(traction):
        mine = traction
        if nblk > 8:
            mine = traction[: 5 * ROWS]
            mine = lax.dynamic_slice_in_dim(mine, blk * 5, 5, 1)
            mine = jnp.pad(mine, ((0, 0), (0, depth - 5)))
        return mine

    def advance(first, last, force, moved, traction, pu, pv, inverse):
        three = shaped(3, N3, ny, depth)
        outs = (three,) * 2 if last else (packed,) * 3 + (face,) * 4 + (packed,) * first
        return call(
            functools.partial(advance_kernel, (ny, nlat, depth), first, last),
            out_shape=outs,
            in_specs=[vmem] * (8 + (not first)),
            out_specs=(vmem,) * len(outs),
            scratch_shapes=[buffer] * (1 if last and not first else 2),
            name="advance",
            cost_estimate=cost(4),
        )(force, *moved, own(traction), pu, pv, *(() if first else (inverse,)))

    pu, pv, force, *rest = advance(True, False, force, moved, traction0, pu, pv, None)
    faces, inverse = rest[:4], rest[4]
    gu, left_seen = lax.optimization_barrier((gu, faces[0]))
    place = pltpu.VMEM((5 * lanes, nlat * fs), jnp.bfloat16)
    gu1, gv1, ginv = call(
        functools.partial(second_interface, dims, npieces),
        out_shape=(wide,) * 3,
        in_specs=[vmem] * (npieces + 2),
        out_specs=(vmem,) * 3,
        scratch_shapes=[pltpu.VMEM((CHUNKS, lanes, 128), f32)] + [held] * 3 + [place],
        name="interface1",
        cost_estimate=cost(4),
    )(*pieces, gu, traction0)
    moved, folded = exchange_lat(*exchange_lon(*faces[:2]), *faces[2:], gv1)
    xv1, folded = lax.optimization_barrier((xv1, folded))
    coef1, xv2, traction1 = call(
        functools.partial(second_traction, dims),
        out_shape=(coefs, xvs, grid_rows),
        in_specs=[vmem] * 10,
        out_specs=(vmem,) * 3,
        scratch_shapes=hats,
        name="traction1",
        cost_estimate=cost(5),
    )(*tables, xv1, hist, gu1, coef0)
    pu, pv, force, *faces = advance(False, False, force, moved, traction1, pu, pv, inverse)
    gu1, left_seen = lax.optimization_barrier((gu1, faces[0]))
    gu2 = call(
        functools.partial(third_interface, dims),
        out_shape=wide,
        in_specs=[vmem] * 4,
        out_specs=vmem,
        scratch_shapes=[held] * 2 + [place],
        name="interface2",
        cost_estimate=cost(4),
    )(gu1, gv1, ginv, traction1)
    moved, folded = exchange_lat(*exchange_lon(*faces[:2]), *faces[2:], gu2)
    xv2, folded = lax.optimization_barrier((xv2, folded))
    xv3, traction2, kept = call(
        functools.partial(third_traction, dims),
        out_shape=(xvs, grid_rows, shaped(3, 3, nown, degrees)),
        in_specs=[vmem] * 11 + [smem],
        out_specs=(vmem,) * 3,
        scratch_shapes=[pltpu.VMEM((6, degrees, degrees), f32)] + hats,
        name="traction2",
        cost_estimate=cost(5),
    )(*tables, xv2, hist, gu2, coef1, coef0, owner_order)
    new_u, new_v = advance(False, True, force, moved, traction2, pu, pv, inverse)
    new_history = jnp.concatenate([kept, past[: lags - 1 - STEPS]], axis=0).transpose(2, 0, 1, 3)
    return (
        new_u.reshape(displacement.shape),
        new_v.reshape(velocity.shape),
        new_history,
        xv3[0:3, 0],
        xv3[3:6, 0],
    )


def solution(mesh):
    field = P(None, None, None, None, "blk", "lat", None)
    nodal = P(None, None, None, "blk", "lat", None)
    columns = P(("blk", "lat"), None, None, None)
    in_specs = (field, field, nodal, nodal, columns, P(), P(), P(), P())
    out_specs = (field, field, columns, P(), P())
    return jax.shard_map(
        functools.partial(on_device, (mesh.shape["blk"], mesh.shape["lat"])),
        mesh=mesh,
        in_specs=in_specs,
        out_specs=out_specs,
        check_vma=False,
    )
```
